128 devices in a mesh: att: 2 (over core), emb: 64 (over z, y, x).
Axes of the slice: x: 4, y: 4, z: 4, core: 2. Of those that a mesh axis runs over, the one named last changes fastest.
Arguments:
- w_qkv: float32 [4, 3, 1024, 1024], P(None, None, 'emb', 'att')
- w_out: float32 [4, 1024, 1024], P(None, 'att', 'emb')
- x_in: bfloat16 [4, 8192, 1024], P(None, None, 'emb')
- dy_qkv: bfloat16 [4, 3, 8192, 1024], P(None, None, None, 'att')
- x_attn: bfloat16 [4, 8192, 1024], P(None, None, 'att')
- dy_out: bfloat16 [4, 8192, 1024], P(None, None, 'emb')
- r_qkv: float32 [4, 3, 1024], P(None, None, 'emb')
- c_qkv: float32 [4, 3, 1024], P(None, None, 'att')
- r_out: float32 [4, 1024], P(None, 'att')
- c_out: float32 [4, 1024], P(None, 'emb')
- hyper_params: float32 [3], replicated
Outputs:
- output 1: float32 [4, 3, 1024, 1024], P(None, None, 'emb', 'att')
- output 2: float32 [4, 1024, 1024], P(None, 'att', 'emb')
- output 3: float32 [4, 3, 1024], P(None, None, 'emb')
- output 4: float32 [4, 3, 1024], P(None, None, 'att')
- output 5: float32 [4, 1024], P(None, 'att')
- output 6: float32 [4, 1024], P(None, 'emb')
All inputs are finite; a program needn't handle non-finite values.
Results may differ from the reference program's by a relative error of at most 0.001.
Values are sent between devices in bfloat16 or wider.
A program may use at most 1 GiB of HBM per device.

```python
import functools
import jax
import jax.numpy as jnp
from jax import lax

D = 1024
HEADS = 16
HEAD = 64
TOKENS = 8192
LAYERS = 4

INNER = HEADS * HEAD
EPS_SQUARE = 1e-30
EPS_SCALE = 1e-3


def cos_scale(rng_key, lead_shape, length, amplitude):
    phase_off = jax.random.uniform(rng_key, lead_shape + (1,), jnp.float32)
    position = jnp.arange(length, dtype=jnp.float32) / length
    return jnp.exp(amplitude * jnp.cos(2.0 * jnp.pi * (position + phase_off)))


def scaled_tokens(rng_key, lead_shape, length, factor):
    key_noise, key_scale = jax.random.split(rng_key)
    gauss_noise = jax.random.normal(key_noise, lead_shape + (2, TOKENS // 2, length), jnp.float32)
    scales = cos_scale(key_scale, lead_shape + (2, 1), length, 0.75)
    return (gauss_noise * scales * factor).reshape(lead_shape + (TOKENS, length)).astype(jnp.bfloat16)


def scaled_weight(rng_key, lead_shape, n_rows, n_cols):
    key_noise, key_row, key_col = jax.random.split(rng_key, 3)
    gauss_noise = jax.random.normal(key_noise, lead_shape + (n_rows, n_cols), jnp.float32)
    row_scale = cos_scale(key_row, lead_shape, n_rows, 0.5)
    col_scale = cos_scale(key_col, lead_shape, n_cols, 0.5)
    return gauss_noise * row_scale[..., :, None] * col_scale[..., None, :] * n_rows ** -0.5


def setup_inputs(seed: int = 0) -> dict:
    key_list = jax.random.split(jax.random.key(seed), 11)
    tok_norm = TOKENS ** -0.5
    low_end = jnp.array([0.5, 0.5, 0.2], jnp.float32)
    high_end = jnp.array([0.8, 1.0, 0.4], jnp.float32)
    return {
        "w_qkv": scaled_weight(key_list[0], (LAYERS, 3), D, INNER),
        "w_out": scaled_weight(key_list[1], (LAYERS,), INNER, D),
        "x_in": scaled_tokens(key_list[2], (LAYERS,), D, 1.0),
        "dy_qkv": scaled_tokens(key_list[3], (LAYERS, 3), INNER, tok_norm),
        "x_attn": scaled_tokens(key_list[4], (LAYERS,), INNER, 1.0),
        "dy_out": scaled_tokens(key_list[5], (LAYERS,), D, tok_norm),
        "r_qkv": jax.random.uniform(key_list[6], (LAYERS, 3, D), jnp.float32, 0.2, 1.0),
        "c_qkv": jax.random.uniform(key_list[7], (LAYERS, 3, INNER), jnp.float32, 0.2, 1.0),
        "r_out": jax.random.uniform(key_list[8], (LAYERS, INNER), jnp.float32, 0.2, 1.0),
        "c_out": jax.random.uniform(key_list[9], (LAYERS, D), jnp.float32, 0.2, 1.0),
        "hyper_params": jax.random.uniform(key_list[10], (3,), jnp.float32, low_end, high_end),
    }


def adafactor_one(w_grad, weight, row_old, col_old, hyper_params):
    beta_two = hyper_params[0]
    rel_step = hyper_params[1]
    clip_limit = hyper_params[2]
    q_sq = w_grad * w_grad + EPS_SQUARE
    row_new = beta_two * row_old + (1.0 - beta_two) * jnp.mean(q_sq, axis=1)
    col_new = beta_two * col_old + (1.0 - beta_two) * jnp.mean(q_sq, axis=0)
    second = row_new[:, None] * col_new[None, :] / jnp.mean(row_new)
    update = w_grad / jnp.sqrt(second)
    rms_u = jnp.sqrt(jnp.mean(update * update))
    clipped = update / jnp.maximum(1.0, rms_u / clip_limit)
    step_size = rel_step * jnp.maximum(EPS_SCALE, jnp.sqrt(jnp.mean(weight * weight)))
    return weight - step_size * clipped, row_new, col_new


def reference(w_qkv, w_out, x_in, dy_qkv, x_attn, dy_out, r_qkv, c_qkv, r_out, c_out, hyper_params):
    step_fn = functools.partial(adafactor_one, hyper_params=hyper_params)

    def one_layer(carry, layer_in):
        lw_qkv, lw_out, lx_in, ldy_qkv, lx_attn, ldy_out, lr_qkv, lc_qkv, lr_out, lc_out = layer_in
        g_qkv = jnp.einsum("td,ktn->kdn", lx_in.astype(jnp.float32), ldy_qkv.astype(jnp.float32))
        g_out = jnp.dot(lx_attn.T, ldy_out, preferred_element_type=jnp.float32)
        new_qkv = jax.vmap(step_fn)(g_qkv, lw_qkv, lr_qkv, lc_qkv)
        new_out = step_fn(g_out, lw_out, lr_out, lc_out)
        return carry, (new_qkv[0], new_out[0], new_qkv[1], new_qkv[2], new_out[1], new_out[2])

    final_carry, results = lax.scan(
        one_layer,
        jnp.zeros((), jnp.float32),
        (w_qkv, w_out, x_in, dy_qkv, x_attn, dy_out, r_qkv, c_qkv, r_out, c_out),
    )
    return (results[0], results[1], results[2], results[3], results[4], results[5])
```

```python
import functools

import jax
import jax.numpy as jnp
from jax import lax
from jax.experimental import pallas as pl
from jax.experimental.pallas import tpu as pltpu
from jax.sharding import PartitionSpec as P

EPS_SQUARE = 1e-30
EPS_SCALE = 1e-3
T_SCALE = 2.0**32

RING = 4
X, Y, Z = 0, 1, 2
STRIDES = (1, 4, 16)

UNITS = (
    (0, 0, X),
    (0, 1, Y),
    (1, 0, Y),
    (1, 1, Z),
    (2, 0, Z),
    (3, 0, X),
    (2, 1, None),
    (3, 1, None),
)
BATCHES = (
    ((0, 0), (0, 1), (0, 2), (0, 3)),
    ((1, 0), (1, 1), (1, 2), (1, 3)),
    ((2, 0), (2, 1), (2, 2)),
    ((3, 0), (3, 1), (3, 2), (2, 3)),
    ((3, 3),),
)
PLAN = (
    ("U", 0), ("U", 1), ("U", 2), ("R", 0), ("U", 3), ("D", 0), ("U", 4), ("R", 1), ("S1", 0), ("U", 5), ("D", 1),
    ("R", 2), ("S2", 0), ("S1", 1), ("D", 2), ("U", 6), ("R", 3), ("F", 0), ("S2", 1), ("S1", 2), ("D", 3),
    ("U", 7), ("R", 4), ("W", 0), ("F", 1), ("S2", 2), ("S1", 3), ("D", 4),
    ("W", 1), ("F", 2), ("S2", 3), ("S1", 4), ("W", 2), ("F", 3), ("S2", 4), ("W", 3), ("F", 4), ("W", 4),
)

GROUPED = tuple(u for u, unit in enumerate(UNITS) if unit[2] is not None)
WHOLE = tuple(u for u, unit in enumerate(UNITS) if unit[2] is None)


def mats_of(unit):
    layer, kind, _ = unit
    return tuple((layer, m) for m in range(3)) if kind == 0 else ((layer, 3),)


GROUPED_MATS = tuple(mat for u in GROUPED for mat in mats_of(UNITS[u]))
AXIS_OF = {mat: UNITS[u][2] for u in GROUPED for mat in mats_of(UNITS[u])}


def kernel(
    tokens, width, att_size,
    w_qkv, w_out, x_in, dy_qkv, x_attn, dy_out, r_qkv, c_qkv, r_out, c_out, hyper,
    w_qkv_new, w_out_new, r_qkv_new, c_qkv_new, r_out_new, c_out_new,
    dy_part, dy_whole, x_part, x_whole, g_part, g_got, g_all, wq, wo, rq, cq, ro, co,
    pair_out, pair_in, stage, fin_out, fin_in,
    small_sem, own_sem, dy_sem, x_send, x_recv, g_send, g_recv, pair_send, pair_recv, st_send, st_recv, fin_send, fin_recv,
    out_sem,
):
    beta_two, rel_step, clip_limit = hyper[0], hyper[1], hyper[2]
    att = lax.axis_index("att")
    emb = lax.axis_index("emb")
    coords = tuple(lax.rem(emb // stride, RING) for stride in STRIDES)
    part = tokens // RING
    n_elems = float(width * width)

    def peer(axis, k):
        place = lax.rem(coords[axis] + k, RING)
        return (att, emb + (place - coords[axis]) * STRIDES[axis]), place

    partner = (lax.rem(att + 1, att_size), emb)

    def remote(src, dst, send, recv, device):
        return pltpu.make_async_remote_copy(
            src_ref=src, dst_ref=dst, send_sem=send, recv_sem=recv, device_id=device, device_id_type=pl.DeviceIdType.MESH
        )

    small = [
        pltpu.make_async_copy(src, dst, small_sem.at[i])
        for i, (src, dst) in enumerate(
            ((w_qkv, wq), (w_out, wo), (r_qkv, rq), (c_qkv, cq), (r_out, ro), (c_out, co))
        )
    ]
    for copy in small:
        copy.start()

    def x_source(u):
        layer, kind, _ = UNITS[u]
        return (x_in, dy_out)[kind].at[layer]

    def x_own(u):
        if u in GROUPED:
            here = coords[UNITS[u][2]]
            src = x_source(u).at[:, pl.ds(pl.multiple_of(here * part, part), part)]
            return pltpu.make_async_copy(src, x_part.at[GROUPED.index(u), here], own_sem.at[u])
        return pltpu.make_async_copy(x_source(u), x_whole.at[WHOLE.index(u)], own_sem.at[u])

    def x_copy(u, k):
        axis = UNITS[u][2]
        device, there = peer(axis, k)
        slot = GROUPED.index(u)
        src = x_source(u).at[:, pl.ds(pl.multiple_of(there * part, part), part)]
        return remote(src, x_part.at[slot, coords[axis]], x_send.at[slot, k - 1], x_recv.at[slot, k - 1], device)

    def dy_source(mat):
        layer, m = mat
        return dy_qkv.at[layer, m] if m < 3 else x_attn.at[layer]

    def dy_copies(u):
        out = []
        for mat in mats_of(UNITS[u]):
            if u in GROUPED:
                i = GROUPED_MATS.index(mat)
                here = coords[UNITS[u][2]]
                src = dy_source(mat).at[pl.ds(pl.multiple_of(here * part, part), part), :]
                out.append(pltpu.make_async_copy(src, dy_part.at[i], dy_sem.at[i]))
            else:
                for j in range(RING):
                    w = WHOLE.index(u)
                    rows = pl.ds(j * part, part)
                    out.append(
                        pltpu.make_async_copy(
                            dy_source(mat).at[rows, :], dy_whole.at[w, rows, :], dy_sem.at[len(GROUPED_MATS) + w * RING + j]
                        )
                    )
        return out

    for u in range(len(UNITS)):
        x_own(u).start()
        for copy in dy_copies(u):
            copy.start()

    barrier = pltpu.get_barrier_semaphore()
    neighbours = [peer(axis, k)[0] for axis in (X, Y, Z) for k in range(1, RING)] + [partner]
    for device in neighbours:
        pl.semaphore_signal(barrier, inc=1, device_id=device, device_id_type=pl.DeviceIdType.MESH)
    pl.semaphore_wait(barrier, len(neighbours))

    for u in GROUPED:
        for k in (1, 3, 2):
            x_copy(u, k).start()

    def g_copy(mat, k):
        axis = AXIS_OF[mat]
        device, there = peer(axis, k)
        i = GROUPED_MATS.index(mat)
        return remote(g_part.at[i, there], g_got.at[i, k - 1], g_send.at[i, k - 1], g_recv.at[i, k - 1], device)

    def slot_of(mat):
        return mat[0] * 4 + mat[1]

    def products(u):
        x_own(u).wait()
        copies = dy_copies(u)
        if u in GROUPED:
            for k in range(1, RING):
                x_copy(u, k).wait_recv()
            lhs = x_part.at[GROUPED.index(u)]
            for mat, copy in zip(mats_of(UNITS[u]), copies):
                i = GROUPED_MATS.index(mat)
                copy.wait()
                got = jnp.dot(
                    lhs[...].reshape(RING * 16, part), dy_part[i], preferred_element_type=jnp.float32
                )
                g_part[i] = got.reshape(RING, 16, got.shape[1])
                for k in range(1, RING):
                    g_copy(mat, k).start()
        else:
            w = WHOLE.index(u)
            (mat,) = mats_of(UNITS[u])
            total = None
            for j, copy in enumerate(copies):
                copy.wait()
                rows = pl.ds(j * part, part)
                got = jnp.dot(x_whole[w, :, rows], dy_whole[w, rows, :], preferred_element_type=jnp.float32)
                total = got if total is None else total + got
            g_all[slot_of(mat)] = total

    diag = lax.broadcasted_iota(jnp.int32, (16, 16), 0) == lax.broadcasted_iota(jnp.int32, (16, 16), 1)
    lane = lax.broadcasted_iota(jnp.int32, (16, 128), 1)

    def up(row):
        return jnp.sum(jnp.where(diag, jnp.broadcast_to(row, (16, 16)), 0.0), axis=1, keepdims=True)

    def across(column):
        return jnp.sum(jnp.where(diag, jnp.broadcast_to(column, (16, 16)), 0.0), axis=0, keepdims=True)

    def pair_copy(b):
        return remote(pair_out.at[b], pair_in.at[b], pair_send.at[b], pair_recv.at[b], partner)

    def stage_copies(b, s):
        here = coords[s]
        out = []
        for k in range(1, RING):
            device, _ = peer(s, k)
            slot = stage.at[b, s, here]
            out.append(remote(slot, slot, st_send.at[b, s, k - 1], st_recv.at[b, s, k - 1], device))
        return out

    def fin_copy(b):
        return remote(fin_out.at[b], fin_in.at[b], fin_send.at[b], fin_recv.at[b], partner)

    def step_r(b):
        tile = jnp.zeros((16, 128), jnp.float32)
        for n, mat in enumerate(BATCHES[b]):
            s = slot_of(mat)
            if mat in GROUPED_MATS:
                i = GROUPED_MATS.index(mat)
                total = g_part[i, coords[AXIS_OF[mat]]]
                for k in range(1, RING):
                    g_copy(mat, k).wait_recv()
                    total = total + g_got[i, k - 1]
                g_all[s] = total
            grad = g_all[s]
            q_sq = grad * grad + EPS_SQUARE
            tile = jnp.where(lane == n, jnp.sum(q_sq, axis=1, keepdims=True), tile)
        pair_out[b] = tile
        pair_copy(b).start()

    def step_d(b):
        here = coords[0]
        mats = BATCHES[b]
        weights = [wo[mat[0]] if mat[1] == 3 else wq[mat[0], mat[1]] for mat in mats]
        w_sq = [jnp.sum(jnp.sum(w * w, axis=0, keepdims=True), axis=1, keepdims=True) for w in weights]
        q_col = []
        for mat in mats:
            grad = g_all[slot_of(mat)]
            q_col.append(jnp.sum(grad * grad + EPS_SQUARE, axis=0, keepdims=True))
        pair_copy(b).wait_recv()
        row_total = pair_out[b] + pair_in[b]
        for n, mat in enumerate(mats):
            layer, m = mat
            s = slot_of(mat)
            old = co[layer : layer + 1, :] if m == 3 else rq[m, layer : layer + 1, :]
            new = beta_two * up(old) + (1.0 - beta_two) * (row_total[:, n : n + 1] / width)
            if m == 3:
                co[layer : layer + 1, :] = across(new)
            else:
                rq[m, layer : layer + 1, :] = across(new)
            t = g_all[s] * lax.rsqrt(new)
            g_all[s] = t
            t_big = t * T_SCALE
            t_col = jnp.sum(t_big * t_big, axis=0, keepdims=True)
            stage[b, 0, here, n : n + 1, 0:512] = q_col[n]
            stage[b, 0, here, n : n + 1, 512:640] = jnp.broadcast_to(jnp.sum(new, axis=0, keepdims=True), (1, 128))
            stage[b, 0, here, 4 + n : 5 + n, 0:512] = t_col
            stage[b, 0, here, 4 + n : 5 + n, 512:640] = jnp.broadcast_to(w_sq[n], (1, 128))
        for n in range(len(mats), 4):
            stage[b, 0, here, n : n + 1, :] = jnp.zeros((1, 640), jnp.float32)
            stage[b, 0, here, 4 + n : 5 + n, :] = jnp.zeros((1, 640), jnp.float32)
        for copy in stage_copies(b, 0):
            copy.start()

    def gather(b, s):
        for copy in stage_copies(b, s):
            copy.wait_recv()
        return (stage[b, s, 0] + stage[b, s, 1]) + (stage[b, s, 2] + stage[b, s, 3])

    def step_s(b, s):
        stage[b, s, coords[s]] = gather(b, s - 1)
        for copy in stage_copies(b, s):
            copy.start()

    sums = {}

    def step_f(b):
        total = gather(b, 2)
        rows = [jnp.zeros((1, 128), jnp.float32)] * 16
        for n, mat in enumerate(BATCHES[b]):
            layer, m = mat
            old = ro[layer : layer + 1, :] if m == 3 else cq[m, layer : layer + 1, :]
            new = beta_two * old + (1.0 - beta_two) * (total[n : n + 1, 0:512] / width)
            if m == 3:
                ro[layer : layer + 1, :] = new
            else:
                cq[m, layer : layer + 1, :] = new
            v = (jnp.sqrt(total[4 + n : 5 + n, 0:512]) * (1.0 / T_SCALE)) * lax.rsqrt(new)
            rows[n] = jnp.broadcast_to(jnp.sum(v * v, axis=1, keepdims=True), (1, 128))
            rows[4 + n] = total[4 + n : 5 + n, 512:640]
            rows[8 + n] = (
                jnp.broadcast_to(jnp.sum(new, axis=1, keepdims=True), (1, 128)) if m == 3 else total[n : n + 1, 512:640] * 0.5
            )
        for i, row in enumerate(rows):
            fin_out[b, i : i + 1, :] = row
        fin_copy(b).start()

    def out_copies(b):
        out = []
        for mat in BATCHES[b]:
            layer, m = mat
            src, dst = (wo.at[layer], w_out_new.at[layer]) if m == 3 else (wq.at[layer, m], w_qkv_new.at[layer, m])
            out.append(pltpu.make_async_copy(src, dst, out_sem.at[slot_of(mat)]))
        return out

    def step_w(b):
        fin_copy(b).wait_recv()
        total = fin_out[b] + fin_in[b]
        for n, mat in enumerate(BATCHES[b]):
            layer, m = mat
            mean_row = total[8 + n : 9 + n, 0:1] / width
            rms_u = jnp.sqrt(mean_row * total[n : n + 1, 0:1] / n_elems)
            rms_w = jnp.sqrt(total[4 + n : 5 + n, 0:1] / n_elems)
            step_size = rel_step * jnp.maximum(EPS_SCALE, rms_w) / jnp.maximum(1.0, rms_u / clip_limit)
            factor = jnp.sqrt(mean_row) * step_size
            j_new = ro[layer : layer + 1, :] if m == 3 else cq[m, layer : layer + 1, :]
            update = (g_all[slot_of(mat)] * lax.rsqrt(j_new)) * factor
            if m == 3:
                wo[layer] = wo[layer] - update
            else:
                wq[layer, m] = wq[layer, m] - update
        for copy in out_copies(b):
            copy.start()

    waited = False
    for what, which in PLAN:
        if what == "U":
            products(which)
        elif what == "R":
            step_r(which)
        elif what == "D":
            if not waited:
                for copy in small:
                    copy.wait()
                waited = True
            step_d(which)
        elif what == "S1":
            step_s(which, 1)
        elif what == "S2":
            step_s(which, 2)
        elif what == "F":
            step_f(which)
        else:
            step_w(which)

    last = [
        pltpu.make_async_copy(src, dst, out_sem.at[16 + i])
        for i, (src, dst) in enumerate(((rq, r_qkv_new), (cq, c_qkv_new), (ro, r_out_new), (co, c_out_new)))
    ]
    for copy in last:
        copy.start()
    for b in range(len(BATCHES)):
        for copy in out_copies(b):
            copy.wait()
    for copy in last:
        copy.wait()
    for u in GROUPED:
        for k in range(1, RING):
            x_copy(u, k).wait_send()
    for mat in GROUPED_MATS:
        for k in range(1, RING):
            g_copy(mat, k).wait_send()
    for b in range(len(BATCHES)):
        pair_copy(b).wait_send()
        fin_copy(b).wait_send()
        for s in range(3):
            for copy in stage_copies(b, s):
                copy.wait_send()


def solution(mesh):
    emb_size = mesh.shape["emb"]
    att_size = mesh.shape["att"]
    in_specs = (
        P(None, None, "emb", "att"),
        P(None, "att", "emb"),
        P(None, None, "emb"),
        P(None, None, None, "att"),
        P(None, None, "att"),
        P(None, None, "emb"),
        P(None, None, "emb"),
        P(None, None, "att"),
        P(None, "att"),
        P(None, "emb"),
        P(),
    )
    out_specs = (
        P(None, None, "emb", "att"),
        P(None, "att", "emb"),
        P(None, None, "emb"),
        P(None, None, "att"),
        P(None, "att"),
        P(None, "emb"),
    )

    def local_run(w_qkv, w_out, x_in, dy_qkv, x_attn, dy_out, r_qkv, c_qkv, r_out, c_out, hyper_params):
        tokens, width = x_in.shape[1], x_in.shape[2] * emb_size
        part = tokens // RING
        w_out = jnp.swapaxes(w_out, 1, 2)
        x_in = jnp.swapaxes(x_in, 1, 2)
        dy_out = jnp.swapaxes(dy_out, 1, 2)
        r_qkv = jnp.swapaxes(r_qkv, 0, 1)
        c_qkv = jnp.swapaxes(c_qkv, 0, 1)
        f32, bf16 = jnp.float32, jnp.bfloat16
        cols = dy_qkv.shape[3]
        n_part, n_whole, n_b = len(GROUPED_MATS), len(WHOLE), len(BATCHES)
        dma = pltpu.SemaphoreType.DMA
        results = (w_qkv, w_out, r_qkv, c_qkv, r_out, c_out)
        out = pl.pallas_call(
            functools.partial(kernel, tokens, width, att_size),
            out_shape=tuple(jax.ShapeDtypeStruct(a.shape, a.dtype) for a in results),
            in_specs=[pl.BlockSpec(memory_space=pl.ANY)] * 10 + [pl.BlockSpec(memory_space=pltpu.SMEM)],
            out_specs=tuple(pl.BlockSpec(memory_space=pl.ANY) for _ in results),
            scratch_shapes=[
                pltpu.VMEM((n_part, part, cols), bf16),
                pltpu.VMEM((n_whole, tokens, cols), bf16),
                pltpu.VMEM((len(GROUPED), RING, 16, part), bf16),
                pltpu.VMEM((n_whole, 16, tokens), bf16),
                pltpu.VMEM((n_part, RING, 16, cols), f32),
                pltpu.VMEM((n_part, RING - 1, 16, cols), f32),
                pltpu.VMEM((16, 16, cols), f32),
                pltpu.VMEM(w_qkv.shape, f32),
                pltpu.VMEM(w_out.shape, f32),
                pltpu.VMEM(r_qkv.shape, f32),
                pltpu.VMEM(c_qkv.shape, f32),
                pltpu.VMEM(r_out.shape, f32),
                pltpu.VMEM(c_out.shape, f32),
                pltpu.VMEM((n_b, 16, 128), f32),
                pltpu.VMEM((n_b, 16, 128), f32),
                pltpu.VMEM((n_b, 3, RING, 8, cols + 128), f32),
                pltpu.VMEM((n_b, 16, 128), f32),
                pltpu.VMEM((n_b, 16, 128), f32),
                dma((6,)),
                dma((len(UNITS),)),
                dma((n_part + n_whole * RING,)),
                dma((len(GROUPED), RING - 1)),
                dma((len(GROUPED), RING - 1)),
                dma((n_part, RING - 1)),
                dma((n_part, RING - 1)),
                dma((n_b,)),
                dma((n_b,)),
                dma((n_b, 3, RING - 1)),
                dma((n_b, 3, RING - 1)),
                dma((n_b,)),
                dma((n_b,)),
                dma((20,)),
            ],
            compiler_params=pltpu.CompilerParams(
                collective_id=0, has_side_effects=True, vmem_limit_bytes=64 * 1024 * 1024 - 64 * 1024
            ),
            name="adafactor",
        )(w_qkv, w_out, x_in, dy_qkv, x_attn, dy_out, r_qkv, c_qkv, r_out, c_out, hyper_params)
        return (
            out[0],
            jnp.swapaxes(out[1], 1, 2),
            jnp.swapaxes(out[2], 0, 1),
            jnp.swapaxes(out[3], 0, 1),
            out[4],
            out[5],
        )

    return jax.shard_map(local_run, mesh=mesh, in_specs=in_specs, out_specs=out_specs, check_vma=False)
```

```python
import functools

import jax
import jax.numpy as jnp
from jax import lax
from jax.experimental import pallas as pl
from jax.experimental.pallas import tpu as pltpu
from jax.sharding import PartitionSpec as P

EPS_SQUARE = 1e-30
EPS_SCALE = 1e-3
T_SCALE = 2.0**32

RING = 4
X, Y, Z = 0, 1, 2
STRIDES = (1, 4, 16)

UNITS = (
    (0, 0, X),
    (0, 1, Y),
    (1, 0, Y),
    (1, 1, Z),
    (2, 0, Z),
    (3, 0, X),
    (2, 1, None),
    (3, 1, None),
)
BATCHES = (
    ((0, 0), (0, 1), (0, 2), (0, 3)),
    ((1, 0), (1, 1), (1, 2), (1, 3)),
    ((2, 0), (2, 1), (2, 2)),
    ((3, 0), (3, 1), (3, 2), (2, 3)),
    ((3, 3),),
)
PLAN = (
    ("U", 0), ("U", 1), ("U", 2), ("R", 0), ("U", 3), ("D", 0), ("U", 4), ("R", 1), ("S1", 0), ("U", 5), ("D", 1),
    ("R", 2), ("S2", 0), ("S1", 1), ("D", 2), ("U", 6), ("R", 3), ("F", 0), ("S2", 1), ("S1", 2), ("D", 3),
    ("U", 7), ("R", 4), ("W", 0), ("F", 1), ("S2", 2), ("S1", 3), ("D", 4),
    ("W", 1), ("F", 2), ("S2", 3), ("S1", 4), ("W", 2), ("F", 3), ("S2", 4), ("W", 3), ("F", 4), ("W", 4),
)

AHEAD_FIRST = 10
AHEAD = 4

GROUPED = tuple(u for u, unit in enumerate(UNITS) if unit[2] is not None)
WHOLE = tuple(u for u, unit in enumerate(UNITS) if unit[2] is None)


def mats_of(unit):
    layer, kind, _ = unit
    return tuple((layer, m) for m in range(3)) if kind == 0 else ((layer, 3),)


GROUPED_MATS = tuple(mat for u in GROUPED for mat in mats_of(UNITS[u]))
AXIS_OF = {mat: UNITS[u][2] for u in GROUPED for mat in mats_of(UNITS[u])}


def kernel(
    tokens, width, att_size,
    w_qkv, w_out, x_in, dy_qkv, x_attn, dy_out, r_qkv, c_qkv, r_out, c_out, hyper,
    w_qkv_new, w_out_new, r_qkv_new, c_qkv_new, r_out_new, c_out_new,
    dy_part, dy_whole, x_full, x_part, g_part, g_got, g_all, wq, wo, rq, cq, ro, co,
    pair_out, pair_in, stage, fin_out, fin_in,
    small_sem, own_sem, dy_sem, x_send, x_recv, g_send, g_recv, pair_send, pair_recv, st_send, st_recv, fin_send, fin_recv,
    out_sem,
):
    beta_two, rel_step, clip_limit = hyper[0], hyper[1], hyper[2]
    att = lax.axis_index("att")
    emb = lax.axis_index("emb")
    coords = tuple(lax.rem(emb // stride, RING) for stride in STRIDES)
    part = tokens // RING
    n_elems = float(width * width)

    def peer(axis, k):
        place = lax.rem(coords[axis] + k, RING)
        return (att, emb + (place - coords[axis]) * STRIDES[axis]), place

    partner = (lax.rem(att + 1, att_size), emb)

    def remote(src, dst, send, recv, device):
        return pltpu.make_async_remote_copy(
            src_ref=src, dst_ref=dst, send_sem=send, recv_sem=recv, device_id=device, device_id_type=pl.DeviceIdType.MESH
        )

    small = [
        pltpu.make_async_copy(src, dst, small_sem.at[i])
        for i, (src, dst) in enumerate(
            ((w_qkv, wq), (w_out, wo), (r_qkv, rq), (c_qkv, cq), (r_out, ro), (c_out, co))
        )
    ]

    def x_source(u):
        layer, kind, _ = UNITS[u]
        return (x_in, dy_out)[kind].at[layer]

    def x_own(u):
        return pltpu.make_async_copy(x_source(u), x_full.at[u], own_sem.at[u])

    def x_copy(u, k):
        axis = UNITS[u][2]
        device, there = peer(axis, k)
        slot = GROUPED.index(u)
        src = x_full.at[u, :, pl.ds(pl.multiple_of(there * part, part), part)]
        return remote(src, x_part.at[slot, coords[axis]], x_send.at[slot, k - 1], x_recv.at[slot, k - 1], device)

    def dy_source(mat):
        layer, m = mat
        return dy_qkv.at[layer, m] if m < 3 else x_attn.at[layer]

    def dy_copies(u):
        out = []
        for mat in mats_of(UNITS[u]):
            if u in GROUPED:
                i = GROUPED_MATS.index(mat)
                here = coords[UNITS[u][2]]
                src = dy_source(mat).at[pl.ds(pl.multiple_of(here * part, part), part), :]
                out.append(pltpu.make_async_copy(src, dy_part.at[i], dy_sem.at[i]))
            else:
                for j in range(RING):
                    w = WHOLE.index(u)
                    rows = pl.ds(j * part, part)
                    out.append(
                        pltpu.make_async_copy(
                            dy_source(mat).at[rows, :], dy_whole.at[w, rows, :], dy_sem.at[len(GROUPED_MATS) + w * RING + j]
                        )
                    )
        return out

    for u in range(len(UNITS)):
        x_own(u).start()
    for copy in small:
        copy.start()
    loads = [copy for u in range(len(UNITS)) for copy in dy_copies(u)]
    started = [0]

    def start_loads(upto):
        for copy in loads[started[0] : upto]:
            copy.start()
        started[0] = max(started[0], min(upto, len(loads)))

    start_loads(AHEAD_FIRST)

    barrier = pltpu.get_barrier_semaphore()
    neighbours = [peer(axis, k)[0] for axis in (X, Y, Z) for k in range(1, RING)] + [partner]
    for device in neighbours:
        pl.semaphore_signal(barrier, inc=1, device_id=device, device_id_type=pl.DeviceIdType.MESH)
    pl.semaphore_wait(barrier, len(neighbours))

    for u in range(len(UNITS)):
        x_own(u).wait()
        if u in GROUPED:
            for k in (1, 3, 2):
                x_copy(u, k).start()
            here = coords[UNITS[u][2]]
            x_part[GROUPED.index(u), here] = x_full[u, :, pl.ds(pl.multiple_of(here * part, part), part)]

    def g_copy(mat, k):
        axis = AXIS_OF[mat]
        device, there = peer(axis, k)
        i = GROUPED_MATS.index(mat)
        return remote(g_part.at[i, there], g_got.at[i, k - 1], g_send.at[i, k - 1], g_recv.at[i, k - 1], device)

    def slot_of(mat):
        return mat[0] * 4 + mat[1]

    done = [0]

    def products(u):
        copies = dy_copies(u)
        if u in GROUPED:
            for k in range(1, RING):
                x_copy(u, k).wait_recv()
            lhs = x_part.at[GROUPED.index(u)]
            for mat, copy in zip(mats_of(UNITS[u]), copies):
                i = GROUPED_MATS.index(mat)
                copy.wait()
                done[0] += 1
                start_loads(done[0] + AHEAD)
                got = jnp.dot(
                    lhs[...].reshape(RING * 16, part), dy_part[i], preferred_element_type=jnp.float32
                )
                g_part[i] = got.reshape(RING, 16, got.shape[1])
                for k in range(1, RING):
                    g_copy(mat, k).start()
        else:
            w = WHOLE.index(u)
            (mat,) = mats_of(UNITS[u])
            total = None
            for j, copy in enumerate(copies):
                copy.wait()
                done[0] += 1
                start_loads(done[0] + AHEAD)
                rows = pl.ds(j * part, part)
                got = jnp.dot(x_full[u, :, rows], dy_whole[w, rows, :], preferred_element_type=jnp.float32)
                total = got if total is None else total + got
            g_all[slot_of(mat)] = total

    diag = lax.broadcasted_iota(jnp.int32, (16, 16), 0) == lax.broadcasted_iota(jnp.int32, (16, 16), 1)
    lane = lax.broadcasted_iota(jnp.int32, (16, 128), 1)

    def up(row):
        return jnp.sum(jnp.where(diag, jnp.broadcast_to(row, (16, 16)), 0.0), axis=1, keepdims=True)

    def across(column):
        return jnp.sum(jnp.where(diag, jnp.broadcast_to(column, (16, 16)), 0.0), axis=0, keepdims=True)

    def pair_copy(b):
        return remote(pair_out.at[b], pair_in.at[b], pair_send.at[b], pair_recv.at[b], partner)

    def stage_copies(b, s):
        here = coords[s]
        out = []
        for k in range(1, RING):
            device, _ = peer(s, k)
            slot = stage.at[b, s, here]
            out.append(remote(slot, slot, st_send.at[b, s, k - 1], st_recv.at[b, s, k - 1], device))
        return out

    def fin_copy(b):
        return remote(fin_out.at[b], fin_in.at[b], fin_send.at[b], fin_recv.at[b], partner)

    def step_r(b):
        tile = jnp.zeros((16, 128), jnp.float32)
        for n, mat in enumerate(BATCHES[b]):
            s = slot_of(mat)
            if mat in GROUPED_MATS:
                i = GROUPED_MATS.index(mat)
                total = g_part[i, coords[AXIS_OF[mat]]]
                for k in range(1, RING):
                    g_copy(mat, k).wait_recv()
                    total = total + g_got[i, k - 1]
                g_all[s] = total
            grad = g_all[s]
            q_sq = grad * grad + EPS_SQUARE
            tile = jnp.where(lane == n, jnp.sum(q_sq, axis=1, keepdims=True), tile)
        pair_out[b] = tile
        pair_copy(b).start()

    def step_d(b):
        here = coords[0]
        mats = BATCHES[b]
        weights = [wo[mat[0]] if mat[1] == 3 else wq[mat[0], mat[1]] for mat in mats]
        w_sq = [jnp.sum(jnp.sum(w * w, axis=0, keepdims=True), axis=1, keepdims=True) for w in weights]
        q_col = []
        for mat in mats:
            grad = g_all[slot_of(mat)]
            q_col.append(jnp.sum(grad * grad + EPS_SQUARE, axis=0, keepdims=True))
        pair_copy(b).wait_recv()
        row_total = pair_out[b] + pair_in[b]
        for n, mat in enumerate(mats):
            layer, m = mat
            s = slot_of(mat)
            old = co[layer : layer + 1, :] if m == 3 else rq[m, layer : layer + 1, :]
            new = beta_two * up(old) + (1.0 - beta_two) * (row_total[:, n : n + 1] / width)
            if m == 3:
                co[layer : layer + 1, :] = across(new)
            else:
                rq[m, layer : layer + 1, :] = across(new)
            t = g_all[s] * lax.rsqrt(new)
            g_all[s] = t
            t_big = t * T_SCALE
            t_col = jnp.sum(t_big * t_big, axis=0, keepdims=True)
            stage[b, 0, here, n : n + 1, 0:512] = q_col[n]
            stage[b, 0, here, n : n + 1, 512:640] = jnp.broadcast_to(jnp.sum(new, axis=0, keepdims=True), (1, 128))
            stage[b, 0, here, 4 + n : 5 + n, 0:512] = t_col
            stage[b, 0, here, 4 + n : 5 + n, 512:640] = jnp.broadcast_to(w_sq[n], (1, 128))
        for n in range(len(mats), 4):
            stage[b, 0, here, n : n + 1, :] = jnp.zeros((1, 640), jnp.float32)
            stage[b, 0, here, 4 + n : 5 + n, :] = jnp.zeros((1, 640), jnp.float32)
        for copy in stage_copies(b, 0):
            copy.start()

    def gather(b, s):
        for copy in stage_copies(b, s):
            copy.wait_recv()
        return (stage[b, s, 0] + stage[b, s, 1]) + (stage[b, s, 2] + stage[b, s, 3])

    def step_s(b, s):
        stage[b, s, coords[s]] = gather(b, s - 1)
        for copy in stage_copies(b, s):
            copy.start()

    sums = {}

    def step_f(b):
        total = gather(b, 2)
        rows = [jnp.zeros((1, 128), jnp.float32)] * 16
        for n, mat in enumerate(BATCHES[b]):
            layer, m = mat
            old = ro[layer : layer + 1, :] if m == 3 else cq[m, layer : layer + 1, :]
            new = beta_two * old + (1.0 - beta_two) * (total[n : n + 1, 0:512] / width)
            if m == 3:
                ro[layer : layer + 1, :] = new
            else:
                cq[m, layer : layer + 1, :] = new
            v = (jnp.sqrt(total[4 + n : 5 + n, 0:512]) * (1.0 / T_SCALE)) * lax.rsqrt(new)
            rows[n] = jnp.broadcast_to(jnp.sum(v * v, axis=1, keepdims=True), (1, 128))
            rows[4 + n] = total[4 + n : 5 + n, 512:640]
            rows[8 + n] = (
                jnp.broadcast_to(jnp.sum(new, axis=1, keepdims=True), (1, 128)) if m == 3 else total[n : n + 1, 512:640] * 0.5
            )
        for i, row in enumerate(rows):
            fin_out[b, i : i + 1, :] = row
        fin_copy(b).start()

    def out_copies(b):
        out = []
        for mat in BATCHES[b]:
            layer, m = mat
            src, dst = (wo.at[layer], w_out_new.at[layer]) if m == 3 else (wq.at[layer, m], w_qkv_new.at[layer, m])
            out.append(pltpu.make_async_copy(src, dst, out_sem.at[slot_of(mat)]))
        return out

    def step_w(b):
        fin_copy(b).wait_recv()
        total = fin_out[b] + fin_in[b]
        for n, mat in enumerate(BATCHES[b]):
            layer, m = mat
            mean_row = total[8 + n : 9 + n, 0:1] / width
            rms_u = jnp.sqrt(mean_row * total[n : n + 1, 0:1] / n_elems)
            rms_w = jnp.sqrt(total[4 + n : 5 + n, 0:1] / n_elems)
            step_size = rel_step * jnp.maximum(EPS_SCALE, rms_w) / jnp.maximum(1.0, rms_u / clip_limit)
            factor = jnp.sqrt(mean_row) * step_size
            j_new = ro[layer : layer + 1, :] if m == 3 else cq[m, layer : layer + 1, :]
            update = (g_all[slot_of(mat)] * lax.rsqrt(j_new)) * factor
            if m == 3:
                wo[layer] = wo[layer] - update
            else:
                wq[layer, m] = wq[layer, m] - update
        for copy in out_copies(b):
            copy.start()

    waited = False
    for what, which in PLAN:
        if what == "U":
            products(which)
        elif what == "R":
            step_r(which)
        elif what == "D":
            if not waited:
                for copy in small:
                    copy.wait()
                waited = True
            step_d(which)
        elif what == "S1":
            step_s(which, 1)
        elif what == "S2":
            step_s(which, 2)
        elif what == "F":
            step_f(which)
        else:
            step_w(which)

    last = [
        pltpu.make_async_copy(src, dst, out_sem.at[16 + i])
        for i, (src, dst) in enumerate(((rq, r_qkv_new), (cq, c_qkv_new), (ro, r_out_new), (co, c_out_new)))
    ]
    for copy in last:
        copy.start()
    for b in range(len(BATCHES)):
        for copy in out_copies(b):
            copy.wait()
    for copy in last:
        copy.wait()
    for u in GROUPED:
        for k in range(1, RING):
            x_copy(u, k).wait_send()
    for mat in GROUPED_MATS:
        for k in range(1, RING):
            g_copy(mat, k).wait_send()
    for b in range(len(BATCHES)):
        pair_copy(b).wait_send()
        fin_copy(b).wait_send()
        for s in range(3):
            for copy in stage_copies(b, s):
                copy.wait_send()


def emit(*refs):
    n = len(refs) // 3
    ins, outs, bufs, sem = refs[:n], refs[n : 2 * n], refs[2 * n : 3 * n], refs[-1]
    for i in range(n):
        pltpu.make_async_copy(ins[i], bufs[i], sem.at[0, i]).start()
    for i in range(n):
        pltpu.make_async_copy(ins[i], bufs[i], sem.at[0, i]).wait()
        pltpu.make_async_copy(bufs[i], outs[i], sem.at[1, i]).start()
    for i in range(n):
        pltpu.make_async_copy(bufs[i], outs[i], sem.at[1, i]).wait()


def solution(mesh):
    emb_size = mesh.shape["emb"]
    att_size = mesh.shape["att"]
    in_specs = (
        P(None, None, "emb", "att"),
        P(None, "att", "emb"),
        P(None, None, "emb"),
        P(None, None, None, "att"),
        P(None, None, "att"),
        P(None, None, "emb"),
        P(None, None, "emb"),
        P(None, None, "att"),
        P(None, "att"),
        P(None, "emb"),
        P(),
    )
    out_specs = (
        P(None, None, "emb", "att"),
        P(None, "att", "emb"),
        P(None, None, "emb"),
        P(None, None, "att"),
        P(None, "att"),
        P(None, "emb"),
    )

    def local_run(w_qkv, w_out, x_in, dy_qkv, x_attn, dy_out, r_qkv, c_qkv, r_out, c_out, hyper_params):
        tokens, width = x_in.shape[1], x_in.shape[2] * emb_size
        part = tokens // RING
        w_out = jnp.swapaxes(w_out, 1, 2)
        x_in = jnp.swapaxes(x_in, 1, 2)
        dy_out = jnp.swapaxes(dy_out, 1, 2)
        r_qkv = jnp.swapaxes(r_qkv, 0, 1)
        c_qkv = jnp.swapaxes(c_qkv, 0, 1)
        f32, bf16 = jnp.float32, jnp.bfloat16
        cols = dy_qkv.shape[3]
        n_part, n_whole, n_b = len(GROUPED_MATS), len(WHOLE), len(BATCHES)
        dma = pltpu.SemaphoreType.DMA
        results = (w_qkv, w_out, r_qkv, c_qkv, r_out, c_out)
        out = pl.pallas_call(
            functools.partial(kernel, tokens, width, att_size),
            out_shape=tuple(jax.ShapeDtypeStruct(a.shape, a.dtype) for a in results),
            in_specs=[pl.BlockSpec(memory_space=pl.ANY)] * 10 + [pl.BlockSpec(memory_space=pltpu.SMEM)],
            out_specs=tuple(pl.BlockSpec(memory_space=pl.ANY) for _ in results),
            scratch_shapes=[
                pltpu.VMEM((n_part, part, cols), bf16),
                pltpu.VMEM((n_whole, tokens, cols), bf16),
                pltpu.VMEM((len(UNITS), 16, tokens), bf16),
                pltpu.VMEM((len(GROUPED), RING, 16, part), bf16),
                pltpu.VMEM((n_part, RING, 16, cols), f32),
                pltpu.VMEM((n_part, RING - 1, 16, cols), f32),
                pltpu.VMEM((16, 16, cols), f32),
                pltpu.VMEM(w_qkv.shape, f32),
                pltpu.VMEM(w_out.shape, f32),
                pltpu.VMEM(r_qkv.shape, f32),
                pltpu.VMEM(c_qkv.shape, f32),
                pltpu.VMEM(r_out.shape, f32),
                pltpu.VMEM(c_out.shape, f32),
                pltpu.VMEM((n_b, 16, 128), f32),
                pltpu.VMEM((n_b, 16, 128), f32),
                pltpu.VMEM((n_b, 3, RING, 8, cols + 128), f32),
                pltpu.VMEM((n_b, 16, 128), f32),
                pltpu.VMEM((n_b, 16, 128), f32),
                dma((6,)),
                dma((len(UNITS),)),
                dma((n_part + n_whole * RING,)),
                dma((len(GROUPED), RING - 1)),
                dma((len(GROUPED), RING - 1)),
                dma((n_part, RING - 1)),
                dma((n_part, RING - 1)),
                dma((n_b,)),
                dma((n_b,)),
                dma((n_b, 3, RING - 1)),
                dma((n_b, 3, RING - 1)),
                dma((n_b,)),
                dma((n_b,)),
                dma((20,)),
            ],
            compiler_params=pltpu.CompilerParams(
                collective_id=0, has_side_effects=True, vmem_limit_bytes=64 * 1024 * 1024 - 64 * 1024
            ),
            name="adafactor",
        )(w_qkv, w_out, x_in, dy_qkv, x_attn, dy_out, r_qkv, c_qkv, r_out, c_out, hyper_params)
        out = pl.pallas_call(
            emit,
            out_shape=tuple(jax.ShapeDtypeStruct(a.shape, a.dtype) for a in out),
            in_specs=[pl.BlockSpec(memory_space=pl.ANY)] * len(out),
            out_specs=tuple(pl.BlockSpec(memory_space=pl.ANY) for _ in out),
            scratch_shapes=[pltpu.VMEM(a.shape, a.dtype) for a in out] + [dma((2, len(out)))],
            name="emit",
        )(*out)
        return (
            out[0],
            jnp.swapaxes(out[1], 1, 2),
            jnp.swapaxes(out[2], 0, 1),
            jnp.swapaxes(out[3], 0, 1),
            out[4],
            out[5],
        )

    return jax.shard_map(local_run, mesh=mesh, in_specs=in_specs, out_specs=out_specs, check_vma=False)
```

```python
import functools

import jax
import jax.numpy as jnp
from jax import lax
from jax.experimental import pallas as pl
from jax.experimental.pallas import tpu as pltpu
from jax.sharding import PartitionSpec as P

EPS_SQUARE = 1e-30
EPS_SCALE = 1e-3
T_SCALE = 2.0**32

RING = 4
X, Y, Z = 0, 1, 2
STRIDES = (1, 4, 16)

SQUARES = (((X, 0), (Y, 0)), ((Y, 1), (Z, 0)), ((Z, 1), (X, 1)))
UNITS = (
    (0, 0, 0),
    (1, 0, 1),
    (2, 0, 2),
    (3, 0, 0),
    (0, 1, 1),
    (1, 1, 2),
    (2, 1, None),
    (3, 1, None),
)
BATCHES = (
    ((0, 0), (0, 1), (0, 2)),
    ((1, 0), (1, 1), (1, 2)),
    ((2, 0), (2, 1), (2, 2)),
    ((3, 0), (3, 1), (3, 2), (0, 3)),
    ((1, 3), (2, 3)),
    ((3, 3),),
)
PLAN = (
    ("U", 0), ("U", 1), ("U", 2), ("R", 0), ("U", 3), ("D", 0), ("R", 1), ("U", 4), ("S1", 0), ("D", 1), ("R", 2), ("U", 5),
    ("S2", 0), ("S1", 1), ("D", 2), ("U", 6), ("R", 3), ("F", 0), ("S2", 1), ("S1", 2), ("D", 3),
    ("R", 4), ("U", 7), ("R", 5), ("W", 0), ("F", 1), ("S2", 2), ("D", 4), ("S1", 3), ("D", 5),
    ("W", 1), ("F", 2), ("S1", 4), ("S2", 3), ("S1", 5), ("W", 2), ("F", 3), ("S2", 4), ("S2", 5),
    ("W", 3), ("F", 4), ("F", 5), ("W", 4), ("W", 5),
)

AHEAD_FIRST = 10
AHEAD = 4

GROUPED = tuple(u for u, unit in enumerate(UNITS) if unit[2] is not None)
WHOLE = tuple(u for u, unit in enumerate(UNITS) if unit[2] is None)


def mats_of(unit):
    layer, kind, _ = unit
    return tuple((layer, m) for m in range(3)) if kind == 0 else ((layer, 3),)


GROUPED_MATS = tuple(mat for u in GROUPED for mat in mats_of(UNITS[u]))
SQUARE_OF = {mat: UNITS[u][2] for u in GROUPED for mat in mats_of(UNITS[u])}


def kernel(
    tokens, width, att_size,
    w_qkv, w_out, x_in, dy_qkv, x_attn, dy_out, r_qkv, c_qkv, r_out, c_out, hyper,
    w_qkv_new, w_out_new, r_qkv_new, c_qkv_new, r_out_new, c_out_new,
    dy_part, dy_whole, x_full, x_part, g_part, g_got, g_all, wq, wo, rq, cq, ro, co,
    pair_out, pair_in, stage, fin_out, fin_in, w_total,
    small_sem, own_sem, dy_sem, x_send, x_recv, g_send, g_recv, pair_send, pair_recv, st_send, st_recv, fin_send, fin_recv,
    out_sem,
):
    beta_two, rel_step, clip_limit = hyper[0], hyper[1], hyper[2]
    att = lax.axis_index("att")
    emb = lax.axis_index("emb")
    coords = tuple(lax.rem(emb // stride, RING) for stride in STRIDES)
    part = tokens // RING
    n_elems = float(width * width)

    def peer(axis, k):
        place = lax.rem(coords[axis] + k, RING)
        return (att, emb + (place - coords[axis]) * STRIDES[axis]), place

    def bit(axis, first):
        return lax.rem(coords[axis] + first, 2)

    def place_in(square):
        (axis_a, first_a), (axis_b, first_b) = SQUARES[square]
        return bit(axis_a, first_a) + 2 * bit(axis_b, first_b)

    def mate(square, k):
        index, place = emb, place_in(square)
        for n, (axis, first) in enumerate(SQUARES[square]):
            if k & (1 << n):
                here = bit(axis, first)
                there = lax.rem(coords[axis] + RING + 1 - 2 * here, RING)
                index = index + (there - coords[axis]) * STRIDES[axis]
                place = place + (1 - 2 * here) * (1 << n)
        return (att, index), place

    partner = (lax.rem(att + 1, att_size), emb)

    def remote(src, dst, send, recv, device):
        return pltpu.make_async_remote_copy(
            src_ref=src, dst_ref=dst, send_sem=send, recv_sem=recv, device_id=device, device_id_type=pl.DeviceIdType.MESH
        )

    small = [
        pltpu.make_async_copy(src, dst, small_sem.at[i])
        for i, (src, dst) in enumerate(
            ((w_qkv, wq), (w_out, wo), (r_qkv, rq), (c_qkv, cq), (r_out, ro), (c_out, co))
        )
    ]

    def x_source(u):
        layer, kind, _ = UNITS[u]
        return (x_in, dy_out)[kind].at[layer]

    def x_own(u):
        return pltpu.make_async_copy(x_source(u), x_full.at[u], own_sem.at[u])

    def x_copy(u, k):
        square = UNITS[u][2]
        device, there = mate(square, k)
        slot = GROUPED.index(u)
        src = x_full.at[u, :, pl.ds(pl.multiple_of(there * part, part), part)]
        return remote(src, x_part.at[slot, place_in(square)], x_send.at[slot, k - 1], x_recv.at[slot, k - 1], device)

    def dy_source(mat):
        layer, m = mat
        return dy_qkv.at[layer, m] if m < 3 else x_attn.at[layer]

    def dy_copies(u):
        out = []
        for mat in mats_of(UNITS[u]):
            if u in GROUPED:
                i = GROUPED_MATS.index(mat)
                here = place_in(UNITS[u][2])
                src = dy_source(mat).at[pl.ds(pl.multiple_of(here * part, part), part), :]
                out.append(pltpu.make_async_copy(src, dy_part.at[i], dy_sem.at[i]))
            else:
                for j in range(RING):
                    w = WHOLE.index(u)
                    rows = pl.ds(j * part, part)
                    out.append(
                        pltpu.make_async_copy(
                            dy_source(mat).at[rows, :], dy_whole.at[w, rows, :], dy_sem.at[len(GROUPED_MATS) + w * RING + j]
                        )
                    )
        return out

    for u in range(len(UNITS)):
        x_own(u).start()
    for copy in small:
        copy.start()
    loads = [copy for u in range(len(UNITS)) for copy in dy_copies(u)]
    started = [0]

    def start_loads(upto):
        for copy in loads[started[0] : upto]:
            copy.start()
        started[0] = max(started[0], min(upto, len(loads)))

    start_loads(AHEAD_FIRST)

    barrier = pltpu.get_barrier_semaphore()
    neighbours = [peer(axis, k)[0] for axis in (X, Y, Z) for k in range(1, RING)] + [partner]
    neighbours += [mate(square, 3)[0] for square in range(len(SQUARES))]
    for device in neighbours:
        pl.semaphore_signal(barrier, inc=1, device_id=device, device_id_type=pl.DeviceIdType.MESH)
    pl.semaphore_wait(barrier, len(neighbours))

    for u in range(len(UNITS)):
        x_own(u).wait()
        if u in GROUPED:
            for k in (3, 1, 2):
                x_copy(u, k).start()
            here = place_in(UNITS[u][2])
            x_part[GROUPED.index(u), here] = x_full[u, :, pl.ds(pl.multiple_of(here * part, part), part)]

    def g_copy(mat, k):
        device, there = mate(SQUARE_OF[mat], k)
        i = GROUPED_MATS.index(mat)
        return remote(g_part.at[i, there], g_got.at[i, k - 1], g_send.at[i, k - 1], g_recv.at[i, k - 1], device)

    def slot_of(mat):
        return mat[0] * 4 + mat[1]

    done = [0]

    def products(u):
        copies = dy_copies(u)
        if u in GROUPED:
            for k in range(1, RING):
                x_copy(u, k).wait_recv()
            lhs = x_part.at[GROUPED.index(u)]
            for mat, copy in zip(mats_of(UNITS[u]), copies):
                i = GROUPED_MATS.index(mat)
                copy.wait()
                done[0] += 1
                start_loads(done[0] + AHEAD)
                got = jnp.dot(
                    lhs[...].reshape(RING * 16, part), dy_part[i], preferred_element_type=jnp.float32
                )
                g_part[i] = got.reshape(RING, 16, got.shape[1])
                for k in range(1, RING):
                    g_copy(mat, k).start()
        else:
            w = WHOLE.index(u)
            (mat,) = mats_of(UNITS[u])
            total = None
            for j, copy in enumerate(copies):
                copy.wait()
                done[0] += 1
                start_loads(done[0] + AHEAD)
                rows = pl.ds(j * part, part)
                got = jnp.dot(x_full[u, :, rows], dy_whole[w, rows, :], preferred_element_type=jnp.float32)
                total = got if total is None else total + got
            g_all[slot_of(mat)] = total

    diag = lax.broadcasted_iota(jnp.int32, (16, 16), 0) == lax.broadcasted_iota(jnp.int32, (16, 16), 1)
    lane = lax.broadcasted_iota(jnp.int32, (16, 128), 1)

    def up(row):
        return jnp.sum(jnp.where(diag, jnp.broadcast_to(row, (16, 16)), 0.0), axis=1, keepdims=True)

    def across(column):
        return jnp.sum(jnp.where(diag, jnp.broadcast_to(column, (16, 16)), 0.0), axis=0, keepdims=True)

    def pair_copy(b):
        return remote(pair_out.at[b], pair_in.at[b], pair_send.at[b], pair_recv.at[b], partner)

    def stage_copies(b, s):
        here = coords[s]
        out = []
        for k in range(1, RING):
            device, _ = peer(s, k)
            slot = stage.at[b, s, here, 0 : rows_of(b), :]
            out.append(remote(slot, slot, st_send.at[b, s, k - 1], st_recv.at[b, s, k - 1], device))
        return out

    def fin_copy(b):
        return remote(fin_out.at[b], fin_in.at[b], fin_send.at[b], fin_recv.at[b], partner)

    def step_r(b):
        tile = jnp.zeros((16, 128), jnp.float32)
        for n, mat in enumerate(BATCHES[b]):
            s = slot_of(mat)
            if mat in GROUPED_MATS:
                i = GROUPED_MATS.index(mat)
                total = g_part[i, place_in(SQUARE_OF[mat])]
                for k in range(1, RING):
                    g_copy(mat, k).wait_recv()
                    total = total + g_got[i, k - 1]
                g_all[s] = total
            grad = g_all[s]
            q_sq = grad * grad + EPS_SQUARE
            tile = jnp.where(lane == n, jnp.sum(q_sq, axis=1, keepdims=True), tile)
        pair_out[b] = tile
        pair_copy(b).start()

    def rows_of(b):
        return 8 * len(BATCHES[b]) + (0 if b == len(BATCHES) - 1 else 8)

    def step_d(b):
        here = coords[0]
        mats = BATCHES[b]
        q_col = []
        for mat in mats:
            grad = g_all[slot_of(mat)]
            q_col.append(jnp.sum(grad * grad + EPS_SQUARE, axis=0, keepdims=True))
        if b == 0:
            w_sq = jnp.zeros((1, 128), jnp.float32)
            for layer in range(4):
                for m in range(4):
                    w = wo[layer] if m == 3 else wq[layer, m]
                    w_sum = jnp.sum(jnp.sum(w * w, axis=0, keepdims=True), axis=1, keepdims=True)
                    w_sq = jnp.where(lane[0:1] == layer * 4 + m, w_sum, w_sq)
        pair_copy(b).wait_recv()
        row_total = pair_out[b] + pair_in[b]
        out = stage.at[b, 0, here]
        for n, mat in enumerate(mats):
            layer, m = mat
            s = slot_of(mat)
            old = co[layer : layer + 1, :] if m == 3 else rq[m, layer : layer + 1, :]
            new = beta_two * up(old) + (1.0 - beta_two) * (row_total[:, n : n + 1] / width)
            if m == 3:
                co[layer : layer + 1, :] = across(new)
            else:
                rq[m, layer : layer + 1, :] = across(new)
            t = g_all[s] * lax.rsqrt(new)
            g_all[s] = t
            t_big = t * T_SCALE
            t_col = jnp.sum(t_big * t_big, axis=0, keepdims=True)
            for i in range(4):
                lanes = slice(128 * i, 128 * i + 128)
                out[8 * n + i : 8 * n + i + 1, :] = q_col[n][:, lanes]
                out[8 * n + 4 + i : 8 * n + 5 + i, :] = t_col[:, lanes]
            if b < len(BATCHES) - 1:
                last = 8 * len(mats) + n
                out[last : last + 1, :] = jnp.broadcast_to(jnp.sum(new, axis=0, keepdims=True), (1, 128))
        if b < len(BATCHES) - 1:
            for n in range(len(mats), 8):
                last = 8 * len(mats) + n
                out[last : last + 1, :] = w_sq if b == 0 and n == 4 else jnp.zeros((1, 128), jnp.float32)
        for copy in stage_copies(b, 0):
            copy.start()

    def gather(b, s):
        for copy in stage_copies(b, s):
            copy.wait_recv()
        part_0, part_1, part_2, part_3 = (stage[b, s, i, 0 : rows_of(b), :] for i in range(RING))
        return (part_0 + part_1) + (part_2 + part_3)

    def step_s(b, s):
        stage[b, s, coords[s], 0 : rows_of(b), :] = gather(b, s - 1)
        for copy in stage_copies(b, s):
            copy.start()

    def step_f(b):
        total = gather(b, 2)
        mats = BATCHES[b]
        for n, mat in enumerate(mats):
            layer, m = mat
            old = ro[layer : layer + 1, :] if m == 3 else cq[m, layer : layer + 1, :]
            q_col, t_col = (
                jnp.concatenate([total[8 * n + 4 * h + i : 8 * n + 4 * h + i + 1, :] for i in range(4)], axis=1)
                for h in range(2)
            )
            new = beta_two * old + (1.0 - beta_two) * (q_col / width)
            if m == 3:
                ro[layer : layer + 1, :] = new
                mean_part = jnp.sum(new, axis=1, keepdims=True)
            else:
                cq[m, layer : layer + 1, :] = new
                mean_part = total[8 * len(mats) + n : 8 * len(mats) + n + 1, 0:1] * 0.5
            v = (jnp.sqrt(t_col) * (1.0 / T_SCALE)) * lax.rsqrt(new)
            fin_out[b, n : n + 1, :] = jnp.broadcast_to(jnp.sum(v * v, axis=1, keepdims=True), (1, 128))
            fin_out[b, 4 + n : 5 + n, :] = jnp.broadcast_to(mean_part, (1, 128))
        for n in range(len(mats), 4):
            fin_out[b, n : n + 1, :] = jnp.zeros((1, 128), jnp.float32)
            fin_out[b, 4 + n : 5 + n, :] = jnp.zeros((1, 128), jnp.float32)
        fin_out[b, 8:16, :] = jnp.zeros((8, 128), jnp.float32)
        if b == 0:
            fin_out[b, 8:9, :] = total[8 * len(mats) + 4 : 8 * len(mats) + 5, :]
        fin_copy(b).start()

    def out_copies(b):
        out = []
        for mat in BATCHES[b]:
            layer, m = mat
            src, dst = (wo.at[layer], w_out_new.at[layer]) if m == 3 else (wq.at[layer, m], w_qkv_new.at[layer, m])
            out.append(pltpu.make_async_copy(src, dst, out_sem.at[slot_of(mat)]))
        return out

    def step_w(b):
        fin_copy(b).wait_recv()
        total = fin_out[b] + fin_in[b]
        if b == 0:
            w_total[...] = total[8:16]
        for n, mat in enumerate(BATCHES[b]):
            layer, m = mat
            mean_row = total[4 + n : 5 + n, 0:1] / width
            rms_u = jnp.sqrt(mean_row * total[n : n + 1, 0:1] / n_elems)
            rms_w = jnp.sqrt(w_total[0:1, slot_of(mat) : slot_of(mat) + 1] / n_elems)
            step_size = rel_step * jnp.maximum(EPS_SCALE, rms_w) / jnp.maximum(1.0, rms_u / clip_limit)
            factor = jnp.sqrt(mean_row) * step_size
            j_new = ro[layer : layer + 1, :] if m == 3 else cq[m, layer : layer + 1, :]
            update = (g_all[slot_of(mat)] * lax.rsqrt(j_new)) * factor
            if m == 3:
                wo[layer] = wo[layer] - update
            else:
                wq[layer, m] = wq[layer, m] - update
        for copy in out_copies(b):
            copy.start()

    waited = False
    for what, which in PLAN:
        if what == "U":
            products(which)
        elif what == "R":
            step_r(which)
        elif what == "D":
            if not waited:
                for copy in small:
                    copy.wait()
                waited = True
            step_d(which)
        elif what == "S1":
            step_s(which, 1)
        elif what == "S2":
            step_s(which, 2)
        elif what == "F":
            step_f(which)
        else:
            step_w(which)

    last = [
        pltpu.make_async_copy(src, dst, out_sem.at[16 + i])
        for i, (src, dst) in enumerate(((rq, r_qkv_new), (cq, c_qkv_new), (ro, r_out_new), (co, c_out_new)))
    ]
    for copy in last:
        copy.start()
    for b in range(len(BATCHES)):
        for copy in out_copies(b):
            copy.wait()
    for copy in last:
        copy.wait()
    for u in GROUPED:
        for k in range(1, RING):
            x_copy(u, k).wait_send()
    for mat in GROUPED_MATS:
        for k in range(1, RING):
            g_copy(mat, k).wait_send()
    for b in range(len(BATCHES)):
        pair_copy(b).wait_send()
        fin_copy(b).wait_send()
        for s in range(3):
            for copy in stage_copies(b, s):
                copy.wait_send()


def emit(*refs):
    n = len(refs) // 3
    ins, outs, bufs, sem = refs[:n], refs[n : 2 * n], refs[2 * n : 3 * n], refs[-1]
    for i in range(n):
        pltpu.make_async_copy(ins[i], bufs[i], sem.at[0, i]).start()
    for i in range(n):
        pltpu.make_async_copy(ins[i], bufs[i], sem.at[0, i]).wait()
        pltpu.make_async_copy(bufs[i], outs[i], sem.at[1, i]).start()
    for i in range(n):
        pltpu.make_async_copy(bufs[i], outs[i], sem.at[1, i]).wait()


def solution(mesh):
    emb_size = mesh.shape["emb"]
    att_size = mesh.shape["att"]
    in_specs = (
        P(None, None, "emb", "att"),
        P(None, "att", "emb"),
        P(None, None, "emb"),
        P(None, None, None, "att"),
        P(None, None, "att"),
        P(None, None, "emb"),
        P(None, None, "emb"),
        P(None, None, "att"),
        P(None, "att"),
        P(None, "emb"),
        P(),
    )
    out_specs = (
        P(None, None, "emb", "att"),
        P(None, "att", "emb"),
        P(None, None, "emb"),
        P(None, None, "att"),
        P(None, "att"),
        P(None, "emb"),
    )

    def local_run(w_qkv, w_out, x_in, dy_qkv, x_attn, dy_out, r_qkv, c_qkv, r_out, c_out, hyper_params):
        tokens, width = x_in.shape[1], x_in.shape[2] * emb_size
        part = tokens // RING
        w_out = jnp.swapaxes(w_out, 1, 2)
        x_in = jnp.swapaxes(x_in, 1, 2)
        dy_out = jnp.swapaxes(dy_out, 1, 2)
        r_qkv = jnp.swapaxes(r_qkv, 0, 1)
        c_qkv = jnp.swapaxes(c_qkv, 0, 1)
        f32, bf16 = jnp.float32, jnp.bfloat16
        cols = dy_qkv.shape[3]
        n_part, n_whole, n_b = len(GROUPED_MATS), len(WHOLE), len(BATCHES)
        dma = pltpu.SemaphoreType.DMA
        results = (w_qkv, w_out, r_qkv, c_qkv, r_out, c_out)
        out = pl.pallas_call(
            functools.partial(kernel, tokens, width, att_size),
            out_shape=tuple(jax.ShapeDtypeStruct(a.shape, a.dtype) for a in results),
            in_specs=[pl.BlockSpec(memory_space=pl.ANY)] * 10 + [pl.BlockSpec(memory_space=pltpu.SMEM)],
            out_specs=tuple(pl.BlockSpec(memory_space=pl.ANY) for _ in results),
            scratch_shapes=[
                pltpu.VMEM((n_part, part, cols), bf16),
                pltpu.VMEM((n_whole, tokens, cols), bf16),
                pltpu.VMEM((len(UNITS), 16, tokens), bf16),
                pltpu.VMEM((len(GROUPED), RING, 16, part), bf16),
                pltpu.VMEM((n_part, RING, 16, cols), f32),
                pltpu.VMEM((n_part, RING - 1, 16, cols), f32),
                pltpu.VMEM((16, 16, cols), f32),
                pltpu.VMEM(w_qkv.shape, f32),
                pltpu.VMEM(w_out.shape, f32),
                pltpu.VMEM(r_qkv.shape, f32),
                pltpu.VMEM(c_qkv.shape, f32),
                pltpu.VMEM(r_out.shape, f32),
                pltpu.VMEM(c_out.shape, f32),
                pltpu.VMEM((n_b, 16, 128), f32),
                pltpu.VMEM((n_b, 16, 128), f32),
                pltpu.VMEM((n_b, 3, RING, 40, 128), f32),
                pltpu.VMEM((n_b, 16, 128), f32),
                pltpu.VMEM((n_b, 16, 128), f32),
                pltpu.VMEM((8, 128), f32),
                dma((6,)),
                dma((len(UNITS),)),
                dma((n_part + n_whole * RING,)),
                dma((len(GROUPED), RING - 1)),
                dma((len(GROUPED), RING - 1)),
                dma((n_part, RING - 1)),
                dma((n_part, RING - 1)),
                dma((n_b,)),
                dma((n_b,)),
                dma((n_b, 3, RING - 1)),
                dma((n_b, 3, RING - 1)),
                dma((n_b,)),
                dma((n_b,)),
                dma((20,)),
            ],
            compiler_params=pltpu.CompilerParams(
                collective_id=0, has_side_effects=True, vmem_limit_bytes=64 * 1024 * 1024 - 64 * 1024
            ),
            name="adafactor",
        )(w_qkv, w_out, x_in, dy_qkv, x_attn, dy_out, r_qkv, c_qkv, r_out, c_out, hyper_params)
        out = pl.pallas_call(
            emit,
            out_shape=tuple(jax.ShapeDtypeStruct(a.shape, a.dtype) for a in out),
            in_specs=[pl.BlockSpec(memory_space=pl.ANY)] * len(out),
            out_specs=tuple(pl.BlockSpec(memory_space=pl.ANY) for _ in out),
            scratch_shapes=[pltpu.VMEM(a.shape, a.dtype) for a in out] + [dma((2, len(out)))],
            name="emit",
        )(*out)
        return (
            out[0],
            jnp.swapaxes(out[1], 1, 2),
            jnp.swapaxes(out[2], 0, 1),
            jnp.swapaxes(out[3], 0, 1),
            out[4],
            out[5],
        )

    return jax.shard_map(local_run, mesh=mesh, in_specs=in_specs, out_specs=out_specs, check_vma=False)
```

```python
import functools

import jax
import jax.numpy as jnp
from jax import lax
from jax.experimental import pallas as pl
from jax.experimental.pallas import tpu as pltpu
from jax.sharding import PartitionSpec as P

EPS_SQUARE = 1e-30
EPS_SCALE = 1e-3
T_SCALE = 2.0**32

RING = 4
X, Y, Z = 0, 1, 2
STRIDES = (1, 4, 16)

SQUARES = (((X, 0), (Y, 0)), ((Y, 1), (Z, 0)), ((Z, 1), (X, 1)))
UNITS = (
    (0, (0, 1, 2), 0),
    (1, (0, 1, 2), 1),
    (2, (0, 1, 2), 2),
    (3, (0,), 0),
    (3, (1,), 1),
    (3, (2,), 2),
    (0, (3,), 0),
    (1, (3,), 1),
    (2, (3,), None),
    (3, (3,), None),
)
BATCHES = (
    ((0, 0), (0, 1), (0, 2), (1, 0), (1, 1), (1, 2)),
    ((2, 0), (2, 1), (2, 2), (3, 0), (2, 3), (3, 3)),
    ((3, 1), (3, 2), (0, 3), (1, 3)),
)
AXES = ((X, Y, Z), (Y, Z, X), (Z, X, Y))
PLAN = (
    ("H", 0), ("H", 1), ("H", 2), ("U", 0), ("H", 3), ("H", 4), ("H", 5), ("U", 1), ("H", 6), ("H", 7), ("U", 2),
    ("U", 3), ("U", 4), ("U", 5), ("U", 6), ("U", 7), ("U", 8), ("R", 0), ("U", 9), ("D", 0), ("R", 1), ("R", 2),
    ("D", 1), ("D", 2), ("S1", 0), ("S1", 1), ("S1", 2), ("S2", 0), ("S2", 1), ("S2", 2), ("F", 0), ("F", 1), ("F", 2),
    ("W", 0), ("W", 1), ("W", 2),
)

AHEAD_FIRST = 3
AHEAD = 4

GROUPED = tuple(u for u, unit in enumerate(UNITS) if unit[2] is not None)
WHOLE = tuple(u for u, unit in enumerate(UNITS) if unit[2] is None)


def mats_of(unit):
    layer, which, _ = unit
    return tuple((layer, m) for m in which)


GROUPED_MATS = tuple(mat for u in GROUPED for mat in mats_of(UNITS[u]))
SQUARE_OF = {mat: UNITS[u][2] for u in GROUPED for mat in mats_of(UNITS[u])}


def kernel(
    tokens, width, att_size,
    w_qkv, w_out, x_in, dy_qkv, x_attn, dy_out, r_qkv, c_qkv, r_out, c_out, hyper,
    w_qkv_new, w_out_new, r_qkv_new, c_qkv_new, r_out_new, c_out_new,
    dy_part, dy_whole, x_full, x_part, g_part, g_got, g_all, wq, wo, rq, cq, ro, co,
    pair_out, pair_in, stage, fin_out, fin_in, w_total, i_stat, j_stat,
    small_sem, own_sem, dy_sem, x_send, x_recv, h_send, h_recv, g_send, g_recv, pair_send, pair_recv, st_send, st_recv, fin_send, fin_recv,
    out_sem,
):
    beta_two, rel_step, clip_limit = hyper[0], hyper[1], hyper[2]
    att = lax.axis_index("att")
    emb = lax.axis_index("emb")
    coords = tuple(lax.rem(emb // stride, RING) for stride in STRIDES)
    part = tokens // RING
    half = part // att_size
    n_elems = float(width * width)

    def peer(axis, k):
        place = lax.rem(coords[axis] + k, RING)
        return (att, emb + (place - coords[axis]) * STRIDES[axis]), place

    def bit(axis, first):
        return lax.rem(coords[axis] + first, 2)

    def place_in(square):
        (axis_a, first_a), (axis_b, first_b) = SQUARES[square]
        return bit(axis_a, first_a) + 2 * bit(axis_b, first_b)

    def mate(square, k):
        index, place = emb, place_in(square)
        for n, (axis, first) in enumerate(SQUARES[square]):
            if k & (1 << n):
                here = bit(axis, first)
                there = lax.rem(coords[axis] + RING + 1 - 2 * here, RING)
                index = index + (there - coords[axis]) * STRIDES[axis]
                place = place + (1 - 2 * here) * (1 << n)
        return (att, index), place

    partner = (lax.rem(att + 1, att_size), emb)

    def remote(src, dst, send, recv, device):
        return pltpu.make_async_remote_copy(
            src_ref=src, dst_ref=dst, send_sem=send, recv_sem=recv, device_id=device, device_id_type=pl.DeviceIdType.MESH
        )

    small = [
        pltpu.make_async_copy(src, dst, small_sem.at[i])
        for i, (src, dst) in enumerate(
            ((w_qkv, wq), (w_out, wo), (r_qkv, rq), (c_qkv, cq), (r_out, ro), (c_out, co))
        )
    ]

    def x_source(u):
        layer, which, _ = UNITS[u]
        return (dy_out if which == (3,) else x_in).at[layer]

    def x_own(u):
        return pltpu.make_async_copy(x_source(u), x_full.at[u], own_sem.at[u])

    def x_copy(u, k):
        square = UNITS[u][2]
        device, there = mate(square, k)
        slot = GROUPED.index(u)
        src = x_full.at[u, :, pl.ds(pl.multiple_of(there * part + att * half, half), half)]
        dst = x_part.at[slot, place_in(square), :, pl.ds(pl.multiple_of(att * half, half), half)]
        return remote(src, dst, x_send.at[slot, k - 1], x_recv.at[slot, k - 1], device)

    def hand_copy(u, k):
        slot = GROUPED.index(u)
        piece = x_part.at[slot, mate(UNITS[u][2], k)[1], :, pl.ds(pl.multiple_of(att * half, half), half)]
        return remote(piece, piece, h_send.at[slot, k - 1], h_recv.at[slot, k - 1], partner)

    def hand(u):
        for k in range(1, RING):
            x_copy(u, k).wait_recv()
            hand_copy(u, k).start()

    def dy_source(mat):
        layer, m = mat
        return dy_qkv.at[layer, m] if m < 3 else x_attn.at[layer]

    def dy_copies(u):
        out = []
        for mat in mats_of(UNITS[u]):
            if u in GROUPED:
                i = GROUPED_MATS.index(mat)
                here = place_in(UNITS[u][2])
                src = dy_source(mat).at[pl.ds(pl.multiple_of(here * part, part), part), :]
                out.append(pltpu.make_async_copy(src, dy_part.at[i], dy_sem.at[i]))
            else:
                for j in range(RING):
                    w = WHOLE.index(u)
                    rows = pl.ds(j * part, part)
                    out.append(
                        pltpu.make_async_copy(
                            dy_source(mat).at[rows, :], dy_whole.at[w, rows, :], dy_sem.at[len(GROUPED_MATS) + w * RING + j]
                        )
                    )
        return out

    for u in range(len(UNITS)):
        x_own(u).start()
    for copy in small:
        copy.start()
    loads = [copy for u in range(len(UNITS)) for copy in dy_copies(u)]
    started = [0]

    def start_loads(upto):
        for copy in loads[started[0] : upto]:
            copy.start()
        started[0] = max(started[0], min(upto, len(loads)))

    start_loads(AHEAD_FIRST)

    barrier = pltpu.get_barrier_semaphore()
    neighbours = [peer(axis, k)[0] for axis in (X, Y, Z) for k in range(1, RING)] + [partner]
    neighbours += [mate(square, 3)[0] for square in range(len(SQUARES))]
    for device in neighbours:
        pl.semaphore_signal(barrier, inc=1, device_id=device, device_id_type=pl.DeviceIdType.MESH)
    pl.semaphore_wait(barrier, len(neighbours))

    for u in range(len(UNITS)):
        x_own(u).wait()
        if u in GROUPED:
            for k in (3, 1, 2):
                x_copy(u, k).start()
            here = place_in(UNITS[u][2])
            x_part[GROUPED.index(u), here] = x_full[u, :, pl.ds(pl.multiple_of(here * part, part), part)]

    start_loads(len(loads))

    def g_copy(mat, k):
        device, there = mate(SQUARE_OF[mat], k)
        i = GROUPED_MATS.index(mat)
        return remote(g_part.at[i, there], g_got.at[i, k - 1], g_send.at[i, k - 1], g_recv.at[i, k - 1], device)

    def slot_of(mat):
        return mat[0] * 4 + mat[1]

    done = [0]

    def products(u):
        copies = dy_copies(u)
        if u in GROUPED:
            for k in range(1, RING):
                hand_copy(u, k).wait_recv()
            lhs = x_part.at[GROUPED.index(u)]
            for mat, copy in zip(mats_of(UNITS[u]), copies):
                i = GROUPED_MATS.index(mat)
                copy.wait()
                done[0] += 1
                start_loads(done[0] + AHEAD)
                got = jnp.dot(
                    lhs[...].reshape(RING * 16, part), dy_part[i], preferred_element_type=jnp.float32
                )
                g_part[i] = got.reshape(RING, 16, got.shape[1])
                for k in range(1, RING):
                    g_copy(mat, k).start()
        else:
            w = WHOLE.index(u)
            (mat,) = mats_of(UNITS[u])
            total = None
            for j, copy in enumerate(copies):
                copy.wait()
                done[0] += 1
                start_loads(done[0] + AHEAD)
                rows = pl.ds(j * part, part)
                got = jnp.dot(x_full[u, :, rows], dy_whole[w, rows, :], preferred_element_type=jnp.float32)
                total = got if total is None else total + got
            g_all[slot_of(mat)] = total

    diag = lax.broadcasted_iota(jnp.int32, (16, 16), 0) == lax.broadcasted_iota(jnp.int32, (16, 16), 1)
    lane = lax.broadcasted_iota(jnp.int32, (16, 128), 1)

    def up(row):
        return jnp.sum(jnp.where(diag, jnp.broadcast_to(row, (16, 16)), 0.0), axis=1, keepdims=True)

    def across(column):
        return jnp.sum(jnp.where(diag, jnp.broadcast_to(column, (16, 16)), 0.0), axis=0, keepdims=True)

    def prepare():
        for b, mats in enumerate(BATCHES):
            tile = jnp.ones((16, 128), jnp.float32)
            for n, (layer, m) in enumerate(mats):
                row = co[layer : layer + 1, :] if m == 3 else rq[m, layer : layer + 1, :]
                tile = jnp.where(lane == n, up(row), tile)
                long = ro[layer : layer + 1, :] if m == 3 else cq[m, layer : layer + 1, :]
                for i in range(4):
                    j_stat[b, 4 * n + i : 4 * n + i + 1, :] = long[:, 128 * i : 128 * i + 128]
            i_stat[b] = tile
        w_sq = jnp.zeros((1, 128), jnp.float32)
        for layer in range(4):
            for m in range(4):
                w = wo[layer] if m == 3 else wq[layer, m]
                w_sum = jnp.sum(jnp.sum(w * w, axis=0, keepdims=True), axis=1, keepdims=True)
                w_sq = jnp.where(lane[0:1] == layer * 4 + m, w_sum, w_sq)
        w_total[0:1, :] = w_sq

    def pair_copy(b):
        return remote(pair_out.at[b], pair_in.at[b], pair_send.at[b], pair_recv.at[b], partner)

    def stage_copies(b, s):
        here = coords[AXES[b][s]]
        out = []
        for k in range(1, RING):
            device, _ = peer(AXES[b][s], k)
            slot = stage.at[b, s, here, 0 : rows_of(b), :]
            out.append(remote(slot, slot, st_send.at[b, s, k - 1], st_recv.at[b, s, k - 1], device))
        return out

    def fin_copy(b):
        rows = 8 * len(BATCHES[b]) + 8
        return remote(fin_out.at[b, 0:rows, :], fin_in.at[b, 0:rows, :], fin_send.at[b], fin_recv.at[b], partner)

    def step_r(b):
        mats = BATCHES[b]
        for mat in mats:
            if mat in GROUPED_MATS:
                for k in range(1, RING):
                    g_copy(mat, k).wait_recv()
        tile = jnp.zeros((16, 128), jnp.float32)
        for n, mat in enumerate(mats):
            s = slot_of(mat)
            if mat in GROUPED_MATS:
                i = GROUPED_MATS.index(mat)
                grad = (g_part[i, place_in(SQUARE_OF[mat])] + g_got[i, 0]) + (g_got[i, 1] + g_got[i, 2])
                g_all[s] = grad
            else:
                grad = g_all[s]
            tile = jnp.where(lane == n, jnp.sum(grad * grad + EPS_SQUARE, axis=1, keepdims=True), tile)
        pair_out[b] = tile
        pair_copy(b).start()
        out = stage.at[b, 0, coords[AXES[b][0]]]
        for n, mat in enumerate(mats):
            grad = g_all[slot_of(mat)]
            q_col = jnp.sum(grad * grad + EPS_SQUARE, axis=0, keepdims=True)
            for i in range(4):
                out[4 * n + i : 4 * n + i + 1, :] = q_col[:, 128 * i : 128 * i + 128]

    def rows_of(b):
        return 8 * len(BATCHES[b]) + 8

    def step_d(b):
        mats = BATCHES[b]
        count = len(mats)
        pair_copy(b).wait_recv()
        new = beta_two * i_stat[b] + (1.0 - beta_two) * ((pair_out[b] + pair_in[b]) / width)
        i_stat[b] = new
        root = lax.rsqrt(new)
        out = stage.at[b, 0, coords[AXES[b][0]]]
        for n, mat in enumerate(mats):
            s = slot_of(mat)
            t = g_all[s] * root[:, n : n + 1]
            g_all[s] = t
            t_big = t * T_SCALE
            t_col = jnp.sum(t_big * t_big, axis=0, keepdims=True)
            for i in range(4):
                row = 4 * (count + n) + i
                out[row : row + 1, :] = t_col[:, 128 * i : 128 * i + 128]
        out[8 * count : 8 * count + 8, :] = jnp.zeros((8, 128), jnp.float32)
        out[8 * count : 8 * count + 1, :] = jnp.sum(new, axis=0, keepdims=True)
        if b == 0:
            out[8 * count + 1 : 8 * count + 2, :] = w_total[0:1, :]
        for copy in stage_copies(b, 0):
            copy.start()

    def gather(b, s):
        for copy in stage_copies(b, s):
            copy.wait_recv()
        part_0, part_1, part_2, part_3 = (stage[b, s, i, 0 : rows_of(b), :] for i in range(RING))
        return (part_0 + part_1) + (part_2 + part_3)

    def step_s(b, s):
        stage[b, s, coords[AXES[b][s]], 0 : rows_of(b), :] = gather(b, s - 1)
        for copy in stage_copies(b, s):
            copy.start()

    def step_f(b):
        count = len(BATCHES[b])
        rows = 4 * count
        total = gather(b, 2)
        new = beta_two * j_stat[b, 0:rows, :] + (1.0 - beta_two) * (total[0:rows] / width)
        v = (jnp.sqrt(total[rows : 2 * rows]) * (1.0 / T_SCALE)) * lax.rsqrt(new)
        fin_out[b, 0:rows, :] = jnp.broadcast_to(jnp.sum(v * v, axis=1, keepdims=True), (rows, 128))
        fin_out[b, rows : 2 * rows, :] = jnp.broadcast_to(jnp.sum(new, axis=1, keepdims=True), (rows, 128))
        fin_out[b, 2 * rows : 2 * rows + 8, :] = total[2 * rows :]
        fin_copy(b).start()
        j_stat[b, 0:rows, :] = new
        for n, (layer, m) in enumerate(BATCHES[b]):
            for i in range(4):
                line = new[4 * n + i : 4 * n + i + 1, :]
                if m == 3:
                    ro[layer : layer + 1, 128 * i : 128 * i + 128] = line
                else:
                    cq[m, layer : layer + 1, 128 * i : 128 * i + 128] = line

    def write_rows():
        for b, mats in enumerate(BATCHES):
            for n, (layer, m) in enumerate(mats):
                line = across(i_stat[b, :, n : n + 1])
                if m == 3:
                    co[layer : layer + 1, :] = line
                else:
                    rq[m, layer : layer + 1, :] = line

    def out_copies(b):
        out = []
        for mat in BATCHES[b]:
            layer, m = mat
            src, dst = (wo.at[layer], w_out_new.at[layer]) if m == 3 else (wq.at[layer, m], w_qkv_new.at[layer, m])
            out.append(pltpu.make_async_copy(src, dst, out_sem.at[slot_of(mat)]))
        return out

    def step_w(b):
        mats = BATCHES[b]
        rows = 4 * len(mats)
        fin_copy(b).wait_recv()
        total = fin_out[b] + fin_in[b]
        if b == 0:
            w_total[...] = total[2 * rows : 2 * rows + 8]

        def four(first):
            return (total[first : first + 1] + total[first + 1 : first + 2]) + (
                total[first + 2 : first + 3] + total[first + 3 : first + 4]
            )

        for n, mat in enumerate(mats):
            layer, m = mat
            if m == 3:
                mean_row = four(rows + 4 * n) / width
            else:
                mean_row = jnp.broadcast_to(fin_out[b, 2 * rows : 2 * rows + 1, n : n + 1] / width, (1, 128))
            rms_u = jnp.sqrt(mean_row * four(4 * n) / n_elems)
            rms_w = jnp.sqrt(w_total[1:2, slot_of(mat) : slot_of(mat) + 1] / n_elems)
            step_size = rel_step * jnp.maximum(EPS_SCALE, rms_w) / jnp.maximum(1.0, rms_u / clip_limit)
            factor = jnp.sqrt(mean_row) * step_size
            scale = lax.rsqrt(j_stat[b, 4 * n : 4 * n + 4, :])
            for i in range(4):
                lanes = slice(128 * i, 128 * i + 128)
                update = (g_all[slot_of(mat), :, lanes] * scale[i : i + 1]) * factor
                if m == 3:
                    wo[layer, :, lanes] = wo[layer, :, lanes] - update
                else:
                    wq[layer, m, :, lanes] = wq[layer, m, :, lanes] - update
        for copy in out_copies(b):
            copy.start()

    statistics = [
        pltpu.make_async_copy(src, dst, out_sem.at[16 + i])
        for i, (src, dst) in enumerate(((rq, r_qkv_new), (cq, c_qkv_new), (ro, r_out_new), (co, c_out_new)))
    ]
    for copy in small:
        copy.wait()
    prepare()
    for what, which in PLAN:
        if what == "H":
            hand(which)
        elif what == "U":
            products(which)
        elif what == "R":
            step_r(which)
        elif what == "D":
            step_d(which)
        elif what == "S1":
            step_s(which, 1)
        elif what == "S2":
            step_s(which, 2)
            if which == len(BATCHES) - 1:
                write_rows()
        elif what == "F":
            step_f(which)
        else:
            if which == 0:
                for copy in statistics:
                    copy.start()
            step_w(which)

    for b in range(len(BATCHES)):
        for copy in out_copies(b):
            copy.wait()
    for copy in statistics:
        copy.wait()
    for u in GROUPED:
        for k in range(1, RING):
            x_copy(u, k).wait_send()
            hand_copy(u, k).wait_send()
    for mat in GROUPED_MATS:
        for k in range(1, RING):
            g_copy(mat, k).wait_send()
    for b in range(len(BATCHES)):
        pair_copy(b).wait_send()
        fin_copy(b).wait_send()
        for s in range(3):
            for copy in stage_copies(b, s):
                copy.wait_send()


def emit(*refs):
    n = len(refs) // 3
    ins, outs, bufs, sem = refs[:n], refs[n : 2 * n], refs[2 * n : 3 * n], refs[-1]
    for i in range(n):
        pltpu.make_async_copy(ins[i], bufs[i], sem.at[0, i]).start()
    for i in range(n):
        pltpu.make_async_copy(ins[i], bufs[i], sem.at[0, i]).wait()
        pltpu.make_async_copy(bufs[i], outs[i], sem.at[1, i]).start()
    for i in range(n):
        pltpu.make_async_copy(bufs[i], outs[i], sem.at[1, i]).wait()


def solution(mesh):
    emb_size = mesh.shape["emb"]
    att_size = mesh.shape["att"]
    in_specs = (
        P(None, None, "emb", "att"),
        P(None, "att", "emb"),
        P(None, None, "emb"),
        P(None, None, None, "att"),
        P(None, None, "att"),
        P(None, None, "emb"),
        P(None, None, "emb"),
        P(None, None, "att"),
        P(None, "att"),
        P(None, "emb"),
        P(),
    )
    out_specs = (
        P(None, None, "emb", "att"),
        P(None, "att", "emb"),
        P(None, None, "emb"),
        P(None, None, "att"),
        P(None, "att"),
        P(None, "emb"),
    )

    def local_run(w_qkv, w_out, x_in, dy_qkv, x_attn, dy_out, r_qkv, c_qkv, r_out, c_out, hyper_params):
        tokens, width = x_in.shape[1], x_in.shape[2] * emb_size
        part = tokens // RING
        w_out = jnp.swapaxes(w_out, 1, 2)
        x_in = jnp.swapaxes(x_in, 1, 2)
        dy_out = jnp.swapaxes(dy_out, 1, 2)
        r_qkv = jnp.swapaxes(r_qkv, 0, 1)
        c_qkv = jnp.swapaxes(c_qkv, 0, 1)
        f32, bf16 = jnp.float32, jnp.bfloat16
        cols = dy_qkv.shape[3]
        n_part, n_whole, n_b = len(GROUPED_MATS), len(WHOLE), len(BATCHES)
        most = 8 * max(len(mats) for mats in BATCHES) + 8
        dma = pltpu.SemaphoreType.DMA
        results = (w_qkv, w_out, r_qkv, c_qkv, r_out, c_out)
        out = pl.pallas_call(
            functools.partial(kernel, tokens, width, att_size),
            out_shape=tuple(jax.ShapeDtypeStruct(a.shape, a.dtype) for a in results),
            in_specs=[pl.BlockSpec(memory_space=pl.ANY)] * 10 + [pl.BlockSpec(memory_space=pltpu.SMEM)],
            out_specs=tuple(pl.BlockSpec(memory_space=pl.ANY) for _ in results),
            scratch_shapes=[
                pltpu.VMEM((n_part, part, cols), bf16),
                pltpu.VMEM((n_whole, tokens, cols), bf16),
                pltpu.VMEM((len(UNITS), 16, tokens), bf16),
                pltpu.VMEM((len(GROUPED), RING, 16, part), bf16),
                pltpu.VMEM((n_part, RING, 16, cols), f32),
                pltpu.VMEM((n_part, RING - 1, 16, cols), f32),
                pltpu.VMEM((16, 16, cols), f32),
                pltpu.VMEM(w_qkv.shape, f32),
                pltpu.VMEM(w_out.shape, f32),
                pltpu.VMEM(r_qkv.shape, f32),
                pltpu.VMEM(c_qkv.shape, f32),
                pltpu.VMEM(r_out.shape, f32),
                pltpu.VMEM(c_out.shape, f32),
                pltpu.VMEM((n_b, 16, 128), f32),
                pltpu.VMEM((n_b, 16, 128), f32),
                pltpu.VMEM((n_b, 3, RING, most, 128), f32),
                pltpu.VMEM((n_b, most, 128), f32),
                pltpu.VMEM((n_b, most, 128), f32),
                pltpu.VMEM((8, 128), f32),
                pltpu.VMEM((n_b, 16, 128), f32),
                pltpu.VMEM((n_b, most, 128), f32),
                dma((6,)),
                dma((len(UNITS),)),
                dma((n_part + n_whole * RING,)),
                dma((len(GROUPED), RING - 1)),
                dma((len(GROUPED), RING - 1)),
                dma((len(GROUPED), RING - 1)),
                dma((len(GROUPED), RING - 1)),
                dma((n_part, RING - 1)),
                dma((n_part, RING - 1)),
                dma((n_b,)),
                dma((n_b,)),
                dma((n_b, 3, RING - 1)),
                dma((n_b, 3, RING - 1)),
                dma((n_b,)),
                dma((n_b,)),
                dma((20,)),
            ],
            compiler_params=pltpu.CompilerParams(
                collective_id=0, has_side_effects=True, vmem_limit_bytes=64 * 1024 * 1024 - 64 * 1024
            ),
            name="adafactor",
        )(w_qkv, w_out, x_in, dy_qkv, x_attn, dy_out, r_qkv, c_qkv, r_out, c_out, hyper_params)
        out = pl.pallas_call(
            emit,
            out_shape=tuple(jax.ShapeDtypeStruct(a.shape, a.dtype) for a in out),
            in_specs=[pl.BlockSpec(memory_space=pl.ANY)] * len(out),
            out_specs=tuple(pl.BlockSpec(memory_space=pl.ANY) for _ in out),
            scratch_shapes=[pltpu.VMEM(a.shape, a.dtype) for a in out] + [dma((2, len(out)))],
            name="emit",
        )(*out)
        return (
            out[0],
            jnp.swapaxes(out[1], 1, 2),
            jnp.swapaxes(out[2], 0, 1),
            jnp.swapaxes(out[3], 0, 1),
            out[4],
            out[5],
        )

    return jax.shard_map(local_run, mesh=mesh, in_specs=in_specs, out_specs=out_specs, check_vma=False)
```

```python
import functools

import jax
import jax.numpy as jnp
from jax import lax
from jax.experimental import pallas as pl
from jax.experimental.pallas import tpu as pltpu
from jax.sharding import PartitionSpec as P

EPS_SQUARE = 1e-30
EPS_SCALE = 1e-3
T_SCALE = 2.0**32

RING = 4
X, Y, Z = 0, 1, 2
STRIDES = (1, 4, 16)

SQUARES = (((X, 0), (Y, 0)), ((Y, 1), (Z, 0)), ((Z, 1), (X, 1)))
UNITS = (
    tuple((layer, (0, 1, 2), layer) for layer in range(3))
    + tuple((3, (m,), m) for m in range(3))
    + tuple((layer, (3,), None) for layer in range(4))
)
PRODUCTS = (
    (((0, 3),),)
    + tuple(tuple((layer, m) for layer in range(3)) for m in range(3))
    + (tuple((3, m) for m in range(3)),)
    + tuple(((layer, 3),) for layer in range(1, 4))
)
READY = PRODUCTS[1] + PRODUCTS[0] + sum(PRODUCTS[2:], ())
BATCHES = tuple(READY[first : first + 4] for first in range(0, len(READY), 4))
CUBES = tuple(tuple((axis, first) for axis in (X, Y, Z)) for first in range(2))
ORDERS = tuple((b % 2, 1 - b % 2) for b in range(len(BATCHES)))
CUBE = 8
PLAN = (
    "U0", "H0", "H1", "H2", "U1", "H3", "H4", "H5", "U2", "U3", "U4", "R0", "U5", "D0", "R1", "U6", "D1", "R2", "U7", "D2",
    "R3", "A0", "D3", "A1", "A2", "F0", "A3", "W0", "F1", "W1", "F2", "W2", "F3", "W3",
)
AHEAD = 3
SLOTS = 26

GROUPED = tuple(u for u, unit in enumerate(UNITS) if unit[2] is not None)
WHOLE = tuple(u for u, unit in enumerate(UNITS) if unit[2] is None)


def mats_of(unit):
    layer, which, _ = unit
    return tuple((layer, m) for m in which)


GROUPED_MATS = tuple(mat for u in GROUPED for mat in mats_of(UNITS[u]))
UNIT_OF = {mat: u for u, unit in enumerate(UNITS) for mat in mats_of(unit)}
BLOCKS = tuple(
    (mat, j) for mats in PRODUCTS for mat in mats for j in ((None,) if mat in GROUPED_MATS else range(RING))
)
SQUARE_OF = {mat: UNITS[u][2] for u in GROUPED for mat in mats_of(UNITS[u])}


def kernel(
    tokens, width, att_size,
    w_qkv, w_out, x_in, dy_qkv, x_attn, dy_out, r_qkv, c_qkv, r_out, c_out, hyper,
    w_qkv_new, w_out_new, r_qkv_new, c_qkv_new, r_out_new, c_out_new,
    dy, x_full, x_part, g_part, g_got, g_all, wq, wo, rq, cq, ro, co,
    pair_out, pair_in, stage, fin_out, fin_in, w_total, i_stat, j_stat,
    small_sem, own_sem, dy_sem, x_send, x_recv, h_send, h_recv, g_send, g_recv, pair_send, pair_recv, st_send, st_recv, fin_send, fin_recv,
    out_sem,
):
    beta_two, rel_step, clip_limit = hyper[0], hyper[1], hyper[2]
    att = lax.axis_index("att")
    emb = lax.axis_index("emb")
    coords = tuple(lax.rem(emb // stride, RING) for stride in STRIDES)
    part = tokens // RING
    half = part // att_size
    n_elems = float(width * width)

    def bit(axis, first):
        return lax.rem(coords[axis] + first, 2)

    def place_in(pairs):
        return sum(bit(axis, first) * (1 << n) for n, (axis, first) in enumerate(pairs))

    def mate(pairs, k):
        index, place = emb, place_in(pairs)
        for n, (axis, first) in enumerate(pairs):
            if k & (1 << n):
                here = bit(axis, first)
                there = lax.rem(coords[axis] + RING + 1 - 2 * here, RING)
                index = index + (there - coords[axis]) * STRIDES[axis]
                place = place + (1 - 2 * here) * (1 << n)
        return (att, index), place

    partner = (lax.rem(att + 1, att_size), emb)

    def remote(src, dst, send, recv, device):
        return pltpu.make_async_remote_copy(
            src_ref=src, dst_ref=dst, send_sem=send, recv_sem=recv, device_id=device, device_id_type=pl.DeviceIdType.MESH
        )

    small = [
        pltpu.make_async_copy(src, dst, small_sem.at[i])
        for i, (src, dst) in enumerate(
            ((w_qkv, wq), (w_out, wo), (r_qkv, rq), (c_qkv, cq), (r_out, ro), (c_out, co))
        )
    ]

    def x_source(u):
        layer, which, _ = UNITS[u]
        return (dy_out if which == (3,) else x_in).at[layer]

    def x_own(u):
        return pltpu.make_async_copy(x_source(u), x_full.at[u], own_sem.at[u])

    def x_copy(u, k):
        square = UNITS[u][2]
        device, there = mate(SQUARES[square], k)
        slot = GROUPED.index(u)
        src = x_full.at[u, :, pl.ds(pl.multiple_of(there * part + att * half, half), half)]
        dst = x_part.at[slot, place_in(SQUARES[square]), :, pl.ds(pl.multiple_of(att * half, half), half)]
        return remote(src, dst, x_send.at[slot, k - 1], x_recv.at[slot, k - 1], device)

    def hand_copy(u, k):
        slot = GROUPED.index(u)
        piece = x_part.at[slot, mate(SQUARES[UNITS[u][2]], k)[1], :, pl.ds(pl.multiple_of(att * half, half), half)]
        return remote(piece, piece, h_send.at[slot, k - 1], h_recv.at[slot, k - 1], partner)

    def hand(u):
        for k in range(1, RING):
            x_copy(u, k).wait_recv()
            hand_copy(u, k).start()

    def dy_source(mat):
        layer, m = mat
        return dy_qkv.at[layer, m] if m < 3 else x_attn.at[layer]

    def dy_copy(c):
        mat, j = BLOCKS[c]
        start = j * part if j is not None else pl.multiple_of(place_in(SQUARES[SQUARE_OF[mat]]) * part, part)
        return pltpu.make_async_copy(dy_source(mat).at[pl.ds(start, part), :], dy.at[c % SLOTS], dy_sem.at[c])

    for u in range(len(UNITS)):
        x_own(u).start()
    for copy in small:
        copy.start()
    started, used = [0], [0]

    def start_loads(upto):
        for c in range(started[0], upto):
            dy_copy(c).start()
        started[0] = max(started[0], upto)

    start_loads(AHEAD)

    barrier = pltpu.get_barrier_semaphore()
    neighbours = [mate(cube, k)[0] for cube in CUBES for k in range(1, CUBE)] + [partner]
    neighbours += [mate(SQUARES[square], 3)[0] for square in range(1, len(SQUARES))]
    for device in neighbours:
        pl.semaphore_signal(barrier, inc=1, device_id=device, device_id_type=pl.DeviceIdType.MESH)
    pl.semaphore_wait(barrier, len(neighbours))

    for u in range(len(UNITS)):
        x_own(u).wait()
        if u in GROUPED:
            for k in (3, 1, 2):
                x_copy(u, k).start()
            here = place_in(SQUARES[UNITS[u][2]])
            x_part[GROUPED.index(u), here] = x_full[u, :, pl.ds(pl.multiple_of(here * part, part), part)]

    start_loads(SLOTS)

    def g_copy(mat, k):
        device, there = mate(SQUARES[SQUARE_OF[mat]], k)
        i = GROUPED_MATS.index(mat)
        return remote(g_part.at[i, there], g_got.at[i, k - 1], g_send.at[i, k - 1], g_recv.at[i, k - 1], device)

    def slot_of(mat):
        return mat[0] * 4 + mat[1]

    handed = set()

    def products(mats):
        u = UNIT_OF[mats[0]]
        first = used[0]
        if u in GROUPED:
            for n, mat in enumerate(mats):
                u = UNIT_OF[mat]
                if u not in handed:
                    handed.add(u)
                    for k in range(1, RING):
                        hand_copy(u, k).wait_recv()
                dy_copy(first + n).wait()
            for n, mat in enumerate(mats):
                i = GROUPED_MATS.index(mat)
                lhs = x_part[GROUPED.index(UNIT_OF[mat])].reshape(RING * 16, part)
                got = jnp.dot(lhs, dy[(first + n) % SLOTS], preferred_element_type=jnp.float32)
                g_part[i] = got.reshape(RING, 16, got.shape[1])
            for mat in mats:
                for k in (3, 1, 2):
                    g_copy(mat, k).start()
            used[0] += len(mats)
        else:
            total = None
            for j in range(RING):
                dy_copy(first + j).wait()
                rows = pl.ds(j * part, part)
                got = jnp.dot(x_full[u, :, rows], dy[(first + j) % SLOTS], preferred_element_type=jnp.float32)
                total = got if total is None else total + got
            g_all[slot_of(mats[0])] = total
            used[0] += RING
        start_loads(min(len(BLOCKS), SLOTS + used[0]))

    diag = lax.broadcasted_iota(jnp.int32, (16, 16), 0) == lax.broadcasted_iota(jnp.int32, (16, 16), 1)
    lane = lax.broadcasted_iota(jnp.int32, (16, 128), 1)

    def up(row):
        return jnp.sum(jnp.where(diag, jnp.broadcast_to(row, (16, 16)), 0.0), axis=1, keepdims=True)

    def across(column):
        return jnp.sum(jnp.where(diag, jnp.broadcast_to(column, (16, 16)), 0.0), axis=0, keepdims=True)

    def prepare():
        for b, mats in enumerate(BATCHES):
            tile = jnp.ones((16, 128), jnp.float32)
            for n, (layer, m) in enumerate(mats):
                row = co[layer : layer + 1, :] if m == 3 else rq[m, layer : layer + 1, :]
                tile = jnp.where(lane == n, up(row), tile)
                long = ro[layer : layer + 1, :] if m == 3 else cq[m, layer : layer + 1, :]
                for i in range(4):
                    j_stat[b, 4 * n + i : 4 * n + i + 1, :] = long[:, 128 * i : 128 * i + 128]
            i_stat[b] = tile
        w_sq = jnp.zeros((1, 128), jnp.float32)
        for layer in range(4):
            for m in range(4):
                w = wo[layer] if m == 3 else wq[layer, m]
                w_sum = jnp.sum(jnp.sum(w * w, axis=0, keepdims=True), axis=1, keepdims=True)
                w_sq = jnp.where(lane[0:1] == layer * 4 + m, w_sum, w_sq)
        w_total[0:1, :] = w_sq

    def pair_copy(b):
        return remote(pair_out.at[b], pair_in.at[b], pair_send.at[b], pair_recv.at[b], partner)

    def stage_copies(b, s):
        here = place_in(CUBES[ORDERS[b][s]])
        out = []
        for k in (7, 6, 5, 3, 4, 2, 1):
            device, _ = mate(CUBES[ORDERS[b][s]], k)
            slot = stage.at[b, s, here, 0 : rows_of(b), :]
            out.append(remote(slot, slot, st_send.at[b, s, k - 1], st_recv.at[b, s, k - 1], device))
        return out

    def fin_copy(b):
        rows = 8 * len(BATCHES[b]) + 8
        return remote(fin_out.at[b, 0:rows, :], fin_in.at[b, 0:rows, :], fin_send.at[b], fin_recv.at[b], partner)

    def step_r(b):
        mats = BATCHES[b]
        for mat in mats:
            if mat in GROUPED_MATS:
                for k in range(1, RING):
                    g_copy(mat, k).wait_recv()
        tile = jnp.zeros((16, 128), jnp.float32)
        for n, mat in enumerate(mats):
            s = slot_of(mat)
            if mat in GROUPED_MATS:
                i = GROUPED_MATS.index(mat)
                grad = (g_part[i, place_in(SQUARES[SQUARE_OF[mat]])] + g_got[i, 0]) + (g_got[i, 1] + g_got[i, 2])
                g_all[s] = grad
            else:
                grad = g_all[s]
            tile = jnp.where(lane == n, jnp.sum(grad * grad + EPS_SQUARE, axis=1, keepdims=True), tile)
        pair_out[b] = tile
        pair_copy(b).start()
        out = stage.at[b, 0, place_in(CUBES[ORDERS[b][0]])]
        for n, mat in enumerate(mats):
            grad = g_all[slot_of(mat)]
            q_col = jnp.sum(grad * grad + EPS_SQUARE, axis=0, keepdims=True)
            for i in range(4):
                out[4 * n + i : 4 * n + i + 1, :] = q_col[:, 128 * i : 128 * i + 128]

    def rows_of(b):
        return 8 * len(BATCHES[b]) + 8

    def step_d(b):
        mats = BATCHES[b]
        count = len(mats)
        pair_copy(b).wait_recv()
        new = beta_two * i_stat[b] + (1.0 - beta_two) * ((pair_out[b] + pair_in[b]) / width)
        i_stat[b] = new
        root = lax.rsqrt(new)
        out = stage.at[b, 0, place_in(CUBES[ORDERS[b][0]])]
        for n, mat in enumerate(mats):
            s = slot_of(mat)
            t = g_all[s] * root[:, n : n + 1]
            g_all[s] = t
            t_big = t * T_SCALE
            t_col = jnp.sum(t_big * t_big, axis=0, keepdims=True)
            for i in range(4):
                row = 4 * (count + n) + i
                out[row : row + 1, :] = t_col[:, 128 * i : 128 * i + 128]
        out[8 * count : 8 * count + 8, :] = jnp.zeros((8, 128), jnp.float32)
        out[8 * count : 8 * count + 1, :] = jnp.sum(new, axis=0, keepdims=True)
        if b == 0:
            out[8 * count + 1 : 8 * count + 2, :] = w_total[0:1, :]
        for copy in stage_copies(b, 0):
            copy.start()

    def gather(b, s):
        for copy in stage_copies(b, s):
            copy.wait_recv()
        parts = [stage[b, s, i, 0 : rows_of(b), :] for i in range(CUBE)]
        while len(parts) > 1:
            parts = [parts[i] + parts[i + 1] for i in range(0, len(parts), 2)]
        return parts[0]

    def step_s(b, s):
        stage[b, s, place_in(CUBES[ORDERS[b][s]]), 0 : rows_of(b), :] = gather(b, s - 1)
        for copy in stage_copies(b, s):
            copy.start()

    def step_f(b):
        count = len(BATCHES[b])
        rows = 4 * count
        total = gather(b, 1)
        new = beta_two * j_stat[b, 0:rows, :] + (1.0 - beta_two) * (total[0:rows] / width)
        v = (jnp.sqrt(total[rows : 2 * rows]) * (1.0 / T_SCALE)) * lax.rsqrt(new)
        fin_out[b, 0:rows, :] = jnp.broadcast_to(jnp.sum(v * v, axis=1, keepdims=True), (rows, 128))
        fin_out[b, rows : 2 * rows, :] = jnp.broadcast_to(jnp.sum(new, axis=1, keepdims=True), (rows, 128))
        fin_out[b, 2 * rows : 2 * rows + 8, :] = total[2 * rows :]
        fin_copy(b).start()
        j_stat[b, 0:rows, :] = new
        for n, (layer, m) in enumerate(BATCHES[b]):
            for i in range(4):
                line = new[4 * n + i : 4 * n + i + 1, :]
                if m == 3:
                    ro[layer : layer + 1, 128 * i : 128 * i + 128] = line
                else:
                    cq[m, layer : layer + 1, 128 * i : 128 * i + 128] = line

    def write_rows():
        for b, mats in enumerate(BATCHES):
            for n, (layer, m) in enumerate(mats):
                line = across(i_stat[b, :, n : n + 1])
                if m == 3:
                    co[layer : layer + 1, :] = line
                else:
                    rq[m, layer : layer + 1, :] = line

    def out_copies(b):
        out = []
        for mat in BATCHES[b]:
            layer, m = mat
            src, dst = (wo.at[layer], w_out_new.at[layer]) if m == 3 else (wq.at[layer, m], w_qkv_new.at[layer, m])
            out.append(pltpu.make_async_copy(src, dst, out_sem.at[slot_of(mat)]))
        return out

    def step_w(b):
        mats = BATCHES[b]
        rows = 4 * len(mats)
        fin_copy(b).wait_recv()
        total = fin_out[b] + fin_in[b]
        if b == 0:
            w_total[...] = total[2 * rows : 2 * rows + 8]

        def four(first):
            return (total[first : first + 1] + total[first + 1 : first + 2]) + (
                total[first + 2 : first + 3] + total[first + 3 : first + 4]
            )

        for n, mat in enumerate(mats):
            layer, m = mat
            if m == 3:
                mean_row = four(rows + 4 * n) / width
            else:
                mean_row = jnp.broadcast_to(fin_out[b, 2 * rows : 2 * rows + 1, n : n + 1] / width, (1, 128))
            rms_u = jnp.sqrt(mean_row * four(4 * n) / n_elems)
            rms_w = jnp.sqrt(w_total[1:2, slot_of(mat) : slot_of(mat) + 1] / n_elems)
            step_size = rel_step * jnp.maximum(EPS_SCALE, rms_w) / jnp.maximum(1.0, rms_u / clip_limit)
            factor = jnp.sqrt(mean_row) * step_size
            scale = lax.rsqrt(j_stat[b, 4 * n : 4 * n + 4, :])
            for i in range(4):
                lanes = slice(128 * i, 128 * i + 128)
                update = (g_all[slot_of(mat), :, lanes] * scale[i : i + 1]) * factor
                if m == 3:
                    wo[layer, :, lanes] = wo[layer, :, lanes] - update
                else:
                    wq[layer, m, :, lanes] = wq[layer, m, :, lanes] - update
        for copy in out_copies(b):
            copy.start()

    statistics = [
        pltpu.make_async_copy(src, dst, out_sem.at[16 + i])
        for i, (src, dst) in enumerate(((rq, r_qkv_new), (cq, c_qkv_new), (ro, r_out_new), (co, c_out_new)))
    ]
    for copy in small:
        copy.wait()
    prepare()
    for step in PLAN:
        what, which = step[0], int(step[1])
        if what == "H":
            hand(which)
        elif what == "U":
            products(PRODUCTS[which])
        elif what == "R":
            step_r(which)
        elif what == "D":
            step_d(which)
        elif what == "A":
            step_s(which, 1)
            if which == len(BATCHES) - 1:
                write_rows()
        elif what == "F":
            step_f(which)
            if which == len(BATCHES) - 1:
                for copy in statistics:
                    copy.start()
        else:
            step_w(which)

    for b in range(len(BATCHES)):
        for copy in out_copies(b):
            copy.wait()
    for copy in statistics:
        copy.wait()
    for u in GROUPED:
        for k in range(1, RING):
            x_copy(u, k).wait_send()
            hand_copy(u, k).wait_send()
    for mat in GROUPED_MATS:
        for k in range(1, RING):
            g_copy(mat, k).wait_send()
    for b in range(len(BATCHES)):
        pair_copy(b).wait_send()
        fin_copy(b).wait_send()
        for s in range(2):
            for copy in stage_copies(b, s):
                copy.wait_send()


def emit(*refs):
    n = len(refs) // 3
    ins, outs, bufs, sem = refs[:n], refs[n : 2 * n], refs[2 * n : 3 * n], refs[-1]
    for i in range(n):
        pltpu.make_async_copy(ins[i], bufs[i], sem.at[0, i]).start()
    for i in range(n):
        pltpu.make_async_copy(ins[i], bufs[i], sem.at[0, i]).wait()
        pltpu.make_async_copy(bufs[i], outs[i], sem.at[1, i]).start()
    for i in range(n):
        pltpu.make_async_copy(bufs[i], outs[i], sem.at[1, i]).wait()


def solution(mesh):
    emb_size = mesh.shape["emb"]
    att_size = mesh.shape["att"]
    in_specs = (
        P(None, None, "emb", "att"),
        P(None, "att", "emb"),
        P(None, None, "emb"),
        P(None, None, None, "att"),
        P(None, None, "att"),
        P(None, None, "emb"),
        P(None, None, "emb"),
        P(None, None, "att"),
        P(None, "att"),
        P(None, "emb"),
        P(),
    )
    out_specs = (
        P(None, None, "emb", "att"),
        P(None, "att", "emb"),
        P(None, None, "emb"),
        P(None, None, "att"),
        P(None, "att"),
        P(None, "emb"),
    )

    def local_run(w_qkv, w_out, x_in, dy_qkv, x_attn, dy_out, r_qkv, c_qkv, r_out, c_out, hyper_params):
        tokens, width = x_in.shape[1], x_in.shape[2] * emb_size
        part = tokens // RING
        w_out = jnp.swapaxes(w_out, 1, 2)
        x_in = jnp.swapaxes(x_in, 1, 2)
        dy_out = jnp.swapaxes(dy_out, 1, 2)
        r_qkv = jnp.swapaxes(r_qkv, 0, 1)
        c_qkv = jnp.swapaxes(c_qkv, 0, 1)
        f32, bf16 = jnp.float32, jnp.bfloat16
        cols = dy_qkv.shape[3]
        n_part, n_b = len(GROUPED_MATS), len(BATCHES)
        most = 8 * max(len(mats) for mats in BATCHES) + 8
        dma = pltpu.SemaphoreType.DMA
        results = (w_qkv, w_out, r_qkv, c_qkv, r_out, c_out)
        out = pl.pallas_call(
            functools.partial(kernel, tokens, width, att_size),
            out_shape=tuple(jax.ShapeDtypeStruct(a.shape, a.dtype) for a in results),
            in_specs=[pl.BlockSpec(memory_space=pl.ANY)] * 10 + [pl.BlockSpec(memory_space=pltpu.SMEM)],
            out_specs=tuple(pl.BlockSpec(memory_space=pl.ANY) for _ in results),
            scratch_shapes=[
                pltpu.VMEM((SLOTS, part, cols), bf16),
                pltpu.VMEM((len(UNITS), 16, tokens), bf16),
                pltpu.VMEM((len(GROUPED), RING, 16, part), bf16),
                pltpu.VMEM((n_part, RING, 16, cols), f32),
                pltpu.VMEM((n_part, RING - 1, 16, cols), f32),
                pltpu.VMEM((16, 16, cols), f32),
                pltpu.VMEM(w_qkv.shape, f32),
                pltpu.VMEM(w_out.shape, f32),
                pltpu.VMEM(r_qkv.shape, f32),
                pltpu.VMEM(c_qkv.shape, f32),
                pltpu.VMEM(r_out.shape, f32),
                pltpu.VMEM(c_out.shape, f32),
                pltpu.VMEM((n_b, 16, 128), f32),
                pltpu.VMEM((n_b, 16, 128), f32),
                pltpu.VMEM((n_b, 2, CUBE, most, 128), f32),
                pltpu.VMEM((n_b, most, 128), f32),
                pltpu.VMEM((n_b, most, 128), f32),
                pltpu.VMEM((8, 128), f32),
                pltpu.VMEM((n_b, 16, 128), f32),
                pltpu.VMEM((n_b, most, 128), f32),
                dma((6,)),
                dma((len(UNITS),)),
                dma((len(BLOCKS),)),
                dma((len(GROUPED), RING - 1)),
                dma((len(GROUPED), RING - 1)),
                dma((len(GROUPED), RING - 1)),
                dma((len(GROUPED), RING - 1)),
                dma((n_part, RING - 1)),
                dma((n_part, RING - 1)),
                dma((n_b,)),
                dma((n_b,)),
                dma((n_b, 2, CUBE - 1)),
                dma((n_b, 2, CUBE - 1)),
                dma((n_b,)),
                dma((n_b,)),
                dma((20,)),
            ],
            compiler_params=pltpu.CompilerParams(
                collective_id=0, has_side_effects=True, vmem_limit_bytes=64 * 1024 * 1024 - 64 * 1024
            ),
            name="adafactor",
        )(w_qkv, w_out, x_in, dy_qkv, x_attn, dy_out, r_qkv, c_qkv, r_out, c_out, hyper_params)
        out = pl.pallas_call(
            emit,
            out_shape=tuple(jax.ShapeDtypeStruct(a.shape, a.dtype) for a in out),
            in_specs=[pl.BlockSpec(memory_space=pl.ANY)] * len(out),
            out_specs=tuple(pl.BlockSpec(memory_space=pl.ANY) for _ in out),
            scratch_shapes=[pltpu.VMEM(a.shape, a.dtype) for a in out] + [dma((2, len(out)))],
            name="emit",
        )(*out)
        return (
            out[0],
            jnp.swapaxes(out[1], 1, 2),
            jnp.swapaxes(out[2], 0, 1),
            jnp.swapaxes(out[3], 0, 1),
            out[4],
            out[5],
        )

    return jax.shard_map(local_run, mesh=mesh, in_specs=in_specs, out_specs=out_specs, check_vma=False)
```

```python
import functools

import jax
import jax.numpy as jnp
from jax import lax
from jax.experimental import pallas as pl
from jax.experimental.pallas import tpu as pltpu
from jax.sharding import PartitionSpec as P

EPS_SQUARE = 1e-30
EPS_SCALE = 1e-3
T_SCALE = 2.0**32

RING = 4
X, Y, Z = 0, 1, 2
STRIDES = (1, 4, 16)

SQUARES = (((X, 0), (Y, 0)), ((Y, 1), (Z, 0)), ((Z, 1), (X, 1)))
UNITS = (
    tuple((layer, (0, 1, 2), layer) for layer in range(3))
    + tuple((3, (m,), m) for m in range(3))
    + tuple((layer, (3,), None) for layer in range(4))
)
PRODUCTS = (
    (((0, 3),),)
    + tuple(tuple((layer, m) for layer in range(3)) for m in range(3))
    + (tuple((3, m) for m in range(3)),)
    + tuple(((layer, 3),) for layer in range(1, 4))
)
READY = PRODUCTS[1] + PRODUCTS[0] + sum(PRODUCTS[2:], ())
BATCHES = tuple(READY[first : first + 4] for first in range(0, len(READY), 4))
CUBES = tuple(tuple((axis, first) for axis in (X, Y, Z)) for first in range(2))
ORDERS = tuple((b % 2, 1 - b % 2) for b in range(len(BATCHES)))
CUBE = 8
PLAN = (
    "U0", "H0", "H1", "H2", "U1", "H3", "H4", "H5", "U2", "U3", "U4", "R0", "U5", "D0", "R1", "U6", "D1", "U7", "R2", "R3",
    "D2", "A0", "D3", "A1", "A2", "F0", "A3", "W0", "F1", "W1", "F2", "W2", "F3", "W3",
)
AHEAD = 3
SLOTS = 26

GROUPED = tuple(u for u, unit in enumerate(UNITS) if unit[2] is not None)
WHOLE = tuple(u for u, unit in enumerate(UNITS) if unit[2] is None)


def mats_of(unit):
    layer, which, _ = unit
    return tuple((layer, m) for m in which)


GROUPED_MATS = tuple(mat for u in GROUPED for mat in mats_of(UNITS[u]))
UNIT_OF = {mat: u for u, unit in enumerate(UNITS) for mat in mats_of(unit)}
BLOCKS = tuple(
    (mat, j) for mats in PRODUCTS for mat in mats for j in ((None,) if mat in GROUPED_MATS else range(RING))
)
SQUARE_OF = {mat: UNITS[u][2] for u in GROUPED for mat in mats_of(UNITS[u])}


def kernel(
    tokens, width, att_size,
    w_qkv, w_out, x_in, dy_qkv, x_attn, dy_out, r_qkv, c_qkv, r_out, c_out, hyper,
    w_qkv_new, w_out_new, r_qkv_new, c_qkv_new, r_out_new, c_out_new,
    dy, x_full, x_part, g_part, g_got, g_all, wq, wo, rq, cq, ro, co,
    pair_out, pair_in, stage, fin_out, fin_in, w_total, i_stat, j_stat,
    small_sem, own_sem, dy_sem, x_send, x_recv, h_send, h_recv, g_send, g_recv, pair_send, pair_recv, st_send, st_recv, fin_send, fin_recv,
    out_sem,
):
    beta_two, rel_step, clip_limit = hyper[0], hyper[1], hyper[2]
    att = lax.axis_index("att")
    emb = lax.axis_index("emb")
    coords = tuple(lax.rem(emb // stride, RING) for stride in STRIDES)
    part = tokens // RING
    half = part // att_size
    n_elems = float(width * width)

    def bit(axis, first):
        return lax.rem(coords[axis] + first, 2)

    def place_in(pairs):
        return sum(bit(axis, first) * (1 << n) for n, (axis, first) in enumerate(pairs))

    def mate(pairs, k):
        index, place = emb, place_in(pairs)
        for n, (axis, first) in enumerate(pairs):
            if k & (1 << n):
                here = bit(axis, first)
                there = lax.rem(coords[axis] + RING + 1 - 2 * here, RING)
                index = index + (there - coords[axis]) * STRIDES[axis]
                place = place + (1 - 2 * here) * (1 << n)
        return (att, index), place

    partner = (lax.rem(att + 1, att_size), emb)

    def remote(src, dst, send, recv, device):
        return pltpu.make_async_remote_copy(
            src_ref=src, dst_ref=dst, send_sem=send, recv_sem=recv, device_id=device, device_id_type=pl.DeviceIdType.MESH
        )

    small = [
        pltpu.make_async_copy(src, dst, small_sem.at[i])
        for i, (src, dst) in enumerate(
            ((w_qkv, wq), (w_out, wo), (r_qkv, rq), (c_qkv, cq), (r_out, ro), (c_out, co))
        )
    ]

    def x_source(u):
        layer, which, _ = UNITS[u]
        return (dy_out if which == (3,) else x_in).at[layer]

    def x_own(u):
        return pltpu.make_async_copy(x_source(u), x_full.at[u], own_sem.at[u])

    def x_copy(u, k):
        square = UNITS[u][2]
        device, there = mate(SQUARES[square], k)
        slot = GROUPED.index(u)
        src = x_full.at[u, :, pl.ds(pl.multiple_of(there * part + att * half, half), half)]
        dst = x_part.at[slot, place_in(SQUARES[square]), :, pl.ds(pl.multiple_of(att * half, half), half)]
        return remote(src, dst, x_send.at[slot, k - 1], x_recv.at[slot, k - 1], device)

    def hand_copy(u, k):
        slot = GROUPED.index(u)
        piece = x_part.at[slot, mate(SQUARES[UNITS[u][2]], k)[1], :, pl.ds(pl.multiple_of(att * half, half), half)]
        return remote(piece, piece, h_send.at[slot, k - 1], h_recv.at[slot, k - 1], partner)

    def hand(u):
        for k in range(1, RING):
            x_copy(u, k).wait_recv()
            hand_copy(u, k).start()

    def dy_source(mat):
        layer, m = mat
        return dy_qkv.at[layer, m] if m < 3 else x_attn.at[layer]

    def dy_copy(c):
        mat, j = BLOCKS[c]
        start = j * part if j is not None else pl.multiple_of(place_in(SQUARES[SQUARE_OF[mat]]) * part, part)
        return pltpu.make_async_copy(dy_source(mat).at[pl.ds(start, part), :], dy.at[c % SLOTS], dy_sem.at[c])

    for u in range(len(UNITS)):
        x_own(u).start()
    for copy in small:
        copy.start()
    started, used = [0], [0]

    def start_loads(upto):
        for c in range(started[0], upto):
            dy_copy(c).start()
        started[0] = max(started[0], upto)

    start_loads(AHEAD)

    barrier = pltpu.get_barrier_semaphore()
    neighbours = [mate(cube, k)[0] for cube in CUBES for k in range(1, CUBE)] + [partner]
    neighbours += [mate(SQUARES[square], 3)[0] for square in range(1, len(SQUARES))]
    for device in neighbours:
        pl.semaphore_signal(barrier, inc=1, device_id=device, device_id_type=pl.DeviceIdType.MESH)
    pl.semaphore_wait(barrier, len(neighbours))

    for u in range(len(UNITS)):
        x_own(u).wait()
        if u in GROUPED:
            for k in (3, 1, 2):
                x_copy(u, k).start()
            here = place_in(SQUARES[UNITS[u][2]])
            x_part[GROUPED.index(u), here] = x_full[u, :, pl.ds(pl.multiple_of(here * part, part), part)]

    start_loads(SLOTS)

    def g_copy(mat, k):
        device, there = mate(SQUARES[SQUARE_OF[mat]], k)
        i = GROUPED_MATS.index(mat)
        return remote(g_part.at[i, there], g_got.at[i, k - 1], g_send.at[i, k - 1], g_recv.at[i, k - 1], device)

    def slot_of(mat):
        return mat[0] * 4 + mat[1]

    handed = set()

    def products(mats):
        u = UNIT_OF[mats[0]]
        first = used[0]
        if u in GROUPED:
            for n, mat in enumerate(mats):
                u = UNIT_OF[mat]
                if u not in handed:
                    handed.add(u)
                    for k in range(1, RING):
                        hand_copy(u, k).wait_recv()
                dy_copy(first + n).wait()
            for n, mat in enumerate(mats):
                i = GROUPED_MATS.index(mat)
                lhs = x_part[GROUPED.index(UNIT_OF[mat])].reshape(RING * 16, part)
                got = jnp.dot(lhs, dy[(first + n) % SLOTS], preferred_element_type=jnp.float32)
                g_part[i] = got.reshape(RING, 16, got.shape[1])
            for mat in mats:
                for k in (3, 1, 2):
                    g_copy(mat, k).start()
            used[0] += len(mats)
        else:
            total = None
            for j in range(RING):
                dy_copy(first + j).wait()
                rows = pl.ds(j * part, part)
                got = jnp.dot(x_full[u, :, rows], dy[(first + j) % SLOTS], preferred_element_type=jnp.float32)
                total = got if total is None else total + got
            g_all[slot_of(mats[0])] = total
            used[0] += RING
        start_loads(min(len(BLOCKS), SLOTS + used[0]))

    diag = lax.broadcasted_iota(jnp.int32, (16, 16), 0) == lax.broadcasted_iota(jnp.int32, (16, 16), 1)
    lane = lax.broadcasted_iota(jnp.int32, (16, 128), 1)

    def up(row):
        return jnp.sum(jnp.where(diag, jnp.broadcast_to(row, (16, 16)), 0.0), axis=1, keepdims=True)

    def across(column):
        return jnp.sum(jnp.where(diag, jnp.broadcast_to(column, (16, 16)), 0.0), axis=0, keepdims=True)

    def prepare():
        for b, mats in enumerate(BATCHES):
            tile = jnp.ones((16, 128), jnp.float32)
            for n, (layer, m) in enumerate(mats):
                row = co[layer : layer + 1, :] if m == 3 else rq[m, layer : layer + 1, :]
                tile = jnp.where(lane == n, up(row), tile)
                long = ro[layer : layer + 1, :] if m == 3 else cq[m, layer : layer + 1, :]
                for i in range(4):
                    j_stat[b, 4 * n + i : 4 * n + i + 1, :] = long[:, 128 * i : 128 * i + 128]
            i_stat[b] = tile
        w_sq = jnp.zeros((1, 128), jnp.float32)
        for layer in range(4):
            for m in range(4):
                w = wo[layer] if m == 3 else wq[layer, m]
                w_sum = jnp.sum(jnp.sum(w * w, axis=0, keepdims=True), axis=1, keepdims=True)
                w_sq = jnp.where(lane[0:1] == layer * 4 + m, w_sum, w_sq)
        w_total[0:1, :] = w_sq

    def pair_copy(b):
        return remote(pair_out.at[b], pair_in.at[b], pair_send.at[b], pair_recv.at[b], partner)

    def stage_copies(b, s):
        here = place_in(CUBES[ORDERS[b][s]])
        out = []
        for k in (7, 6, 5, 3, 4, 2, 1):
            device, _ = mate(CUBES[ORDERS[b][s]], k)
            slot = stage.at[b, s, here, 0 : rows_of(b), :]
            out.append(remote(slot, slot, st_send.at[b, s, k - 1], st_recv.at[b, s, k - 1], device))
        return out

    def fin_copy(b):
        rows = 8 * len(BATCHES[b]) + 8
        return remote(fin_out.at[b, 0:rows, :], fin_in.at[b, 0:rows, :], fin_send.at[b], fin_recv.at[b], partner)

    def step_r(b):
        mats = BATCHES[b]
        for mat in mats:
            if mat in GROUPED_MATS:
                for k in range(1, RING):
                    g_copy(mat, k).wait_recv()
        tile = jnp.zeros((16, 128), jnp.float32)
        for n, mat in enumerate(mats):
            s = slot_of(mat)
            if mat in GROUPED_MATS:
                i = GROUPED_MATS.index(mat)
                grad = (g_part[i, place_in(SQUARES[SQUARE_OF[mat]])] + g_got[i, 0]) + (g_got[i, 1] + g_got[i, 2])
                g_all[s] = grad
            else:
                grad = g_all[s]
            tile = jnp.where(lane == n, jnp.sum(grad * grad + EPS_SQUARE, axis=1, keepdims=True), tile)
        pair_out[b] = tile
        pair_copy(b).start()
        out = stage.at[b, 0, place_in(CUBES[ORDERS[b][0]])]
        for n, mat in enumerate(mats):
            grad = g_all[slot_of(mat)]
            q_col = jnp.sum(grad * grad + EPS_SQUARE, axis=0, keepdims=True)
            for i in range(4):
                out[4 * n + i : 4 * n + i + 1, :] = q_col[:, 128 * i : 128 * i + 128]

    def rows_of(b):
        return 8 * len(BATCHES[b]) + 8

    def step_d(b):
        mats = BATCHES[b]
        count = len(mats)
        pair_copy(b).wait_recv()
        new = beta_two * i_stat[b] + (1.0 - beta_two) * ((pair_out[b] + pair_in[b]) / width)
        i_stat[b] = new
        root = lax.rsqrt(new)
        out = stage.at[b, 0, place_in(CUBES[ORDERS[b][0]])]
        for n, mat in enumerate(mats):
            s = slot_of(mat)
            t = g_all[s] * root[:, n : n + 1]
            g_all[s] = t
            t_big = t * T_SCALE
            t_col = jnp.sum(t_big * t_big, axis=0, keepdims=True)
            for i in range(4):
                row = 4 * (count + n) + i
                out[row : row + 1, :] = t_col[:, 128 * i : 128 * i + 128]
        out[8 * count : 8 * count + 8, :] = jnp.zeros((8, 128), jnp.float32)
        out[8 * count : 8 * count + 1, :] = jnp.sum(new, axis=0, keepdims=True)
        if b == 0:
            out[8 * count + 1 : 8 * count + 2, :] = w_total[0:1, :]
        for copy in stage_copies(b, 0):
            copy.start()

    def gather(b, s):
        for copy in stage_copies(b, s):
            copy.wait_recv()
        parts = [stage[b, s, i, 0 : rows_of(b), :] for i in range(CUBE)]
        while len(parts) > 1:
            parts = [parts[i] + parts[i + 1] for i in range(0, len(parts), 2)]
        return parts[0]

    def step_s(b, s):
        stage[b, s, place_in(CUBES[ORDERS[b][s]]), 0 : rows_of(b), :] = gather(b, s - 1)
        for copy in stage_copies(b, s):
            copy.start()

    def step_f(b):
        count = len(BATCHES[b])
        rows = 4 * count
        total = gather(b, 1)
        new = beta_two * j_stat[b, 0:rows, :] + (1.0 - beta_two) * (total[0:rows] / width)
        v = (jnp.sqrt(total[rows : 2 * rows]) * (1.0 / T_SCALE)) * lax.rsqrt(new)
        fin_out[b, 0:rows, :] = jnp.broadcast_to(jnp.sum(v * v, axis=1, keepdims=True), (rows, 128))
        fin_out[b, rows : 2 * rows, :] = jnp.broadcast_to(jnp.sum(new, axis=1, keepdims=True), (rows, 128))
        fin_out[b, 2 * rows : 2 * rows + 8, :] = total[2 * rows :]
        fin_copy(b).start()
        j_stat[b, 0:rows, :] = new
        for n, (layer, m) in enumerate(BATCHES[b]):
            for i in range(4):
                line = new[4 * n + i : 4 * n + i + 1, :]
                if m == 3:
                    ro[layer : layer + 1, 128 * i : 128 * i + 128] = line
                else:
                    cq[m, layer : layer + 1, 128 * i : 128 * i + 128] = line

    def write_rows():
        for b, mats in enumerate(BATCHES):
            for n, (layer, m) in enumerate(mats):
                line = across(i_stat[b, :, n : n + 1])
                if m == 3:
                    co[layer : layer + 1, :] = line
                else:
                    rq[m, layer : layer + 1, :] = line

    def out_copies(b):
        out = []
        for mat in BATCHES[b]:
            layer, m = mat
            src, dst = (wo.at[layer], w_out_new.at[layer]) if m == 3 else (wq.at[layer, m], w_qkv_new.at[layer, m])
            out.append(pltpu.make_async_copy(src, dst, out_sem.at[slot_of(mat)]))
        return out

    def step_w(b):
        mats = BATCHES[b]
        rows = 4 * len(mats)
        fin_copy(b).wait_recv()
        total = fin_out[b] + fin_in[b]
        if b == 0:
            w_total[...] = total[2 * rows : 2 * rows + 8]

        def four(first):
            return (total[first : first + 1] + total[first + 1 : first + 2]) + (
                total[first + 2 : first + 3] + total[first + 3 : first + 4]
            )

        for n, mat in enumerate(mats):
            layer, m = mat
            if m == 3:
                mean_row = four(rows + 4 * n) / width
            else:
                mean_row = jnp.broadcast_to(fin_out[b, 2 * rows : 2 * rows + 1, n : n + 1] / width, (1, 128))
            rms_u = jnp.sqrt(mean_row * four(4 * n) / n_elems)
            rms_w = jnp.sqrt(w_total[1:2, slot_of(mat) : slot_of(mat) + 1] / n_elems)
            step_size = rel_step * jnp.maximum(EPS_SCALE, rms_w) / jnp.maximum(1.0, rms_u / clip_limit)
            factor = jnp.sqrt(mean_row) * step_size
            scale = lax.rsqrt(j_stat[b, 4 * n : 4 * n + 4, :])
            for i in range(4):
                lanes = slice(128 * i, 128 * i + 128)
                update = (g_all[slot_of(mat), :, lanes] * scale[i : i + 1]) * factor
                if m == 3:
                    wo[layer, :, lanes] = wo[layer, :, lanes] - update
                else:
                    wq[layer, m, :, lanes] = wq[layer, m, :, lanes] - update
        for copy in out_copies(b):
            copy.start()

    statistics = [
        pltpu.make_async_copy(src, dst, out_sem.at[16 + i])
        for i, (src, dst) in enumerate(((rq, r_qkv_new), (cq, c_qkv_new), (ro, r_out_new), (co, c_out_new)))
    ]
    for copy in small:
        copy.wait()
    prepare()
    for step in PLAN:
        what, which = step[0], int(step[1])
        if what == "H":
            hand(which)
        elif what == "U":
            products(PRODUCTS[which])
        elif what == "R":
            step_r(which)
        elif what == "D":
            step_d(which)
        elif what == "A":
            step_s(which, 1)
            if which == len(BATCHES) - 1:
                write_rows()
        elif what == "F":
            step_f(which)
            if which == len(BATCHES) - 1:
                for copy in statistics:
                    copy.start()
        else:
            step_w(which)

    for b in range(len(BATCHES)):
        for copy in out_copies(b):
            copy.wait()
    for copy in statistics:
        copy.wait()
    for u in GROUPED:
        for k in range(1, RING):
            x_copy(u, k).wait_send()
            hand_copy(u, k).wait_send()
    for mat in GROUPED_MATS:
        for k in range(1, RING):
            g_copy(mat, k).wait_send()
    for b in range(len(BATCHES)):
        pair_copy(b).wait_send()
        fin_copy(b).wait_send()
        for s in range(2):
            for copy in stage_copies(b, s):
                copy.wait_send()


def emit(*refs):
    n = len(refs) // 3
    ins, outs, bufs, sem = refs[:n], refs[n : 2 * n], refs[2 * n : 3 * n], refs[-1]
    for i in range(n):
        pltpu.make_async_copy(ins[i], bufs[i], sem.at[0, i]).start()
    for i in range(n):
        pltpu.make_async_copy(ins[i], bufs[i], sem.at[0, i]).wait()
        pltpu.make_async_copy(bufs[i], outs[i], sem.at[1, i]).start()
    for i in range(n):
        pltpu.make_async_copy(bufs[i], outs[i], sem.at[1, i]).wait()


def solution(mesh):
    emb_size = mesh.shape["emb"]
    att_size = mesh.shape["att"]
    in_specs = (
        P(None, None, "emb", "att"),
        P(None, "att", "emb"),
        P(None, None, "emb"),
        P(None, None, None, "att"),
        P(None, None, "att"),
        P(None, None, "emb"),
        P(None, None, "emb"),
        P(None, None, "att"),
        P(None, "att"),
        P(None, "emb"),
        P(),
    )
    out_specs = (
        P(None, None, "emb", "att"),
        P(None, "att", "emb"),
        P(None, None, "emb"),
        P(None, None, "att"),
        P(None, "att"),
        P(None, "emb"),
    )

    def local_run(w_qkv, w_out, x_in, dy_qkv, x_attn, dy_out, r_qkv, c_qkv, r_out, c_out, hyper_params):
        tokens, width = x_in.shape[1], x_in.shape[2] * emb_size
        part = tokens // RING
        w_out = jnp.swapaxes(w_out, 1, 2)
        x_in = jnp.swapaxes(x_in, 1, 2)
        dy_out = jnp.swapaxes(dy_out, 1, 2)
        r_qkv = jnp.swapaxes(r_qkv, 0, 1)
        c_qkv = jnp.swapaxes(c_qkv, 0, 1)
        f32, bf16 = jnp.float32, jnp.bfloat16
        cols = dy_qkv.shape[3]
        n_part, n_b = len(GROUPED_MATS), len(BATCHES)
        most = 8 * max(len(mats) for mats in BATCHES) + 8
        dma = pltpu.SemaphoreType.DMA
        results = (w_qkv, w_out, r_qkv, c_qkv, r_out, c_out)
        out = pl.pallas_call(
            functools.partial(kernel, tokens, width, att_size),
            out_shape=tuple(jax.ShapeDtypeStruct(a.shape, a.dtype) for a in results),
            in_specs=[pl.BlockSpec(memory_space=pl.ANY)] * 10 + [pl.BlockSpec(memory_space=pltpu.SMEM)],
            out_specs=tuple(pl.BlockSpec(memory_space=pl.ANY) for _ in results),
            scratch_shapes=[
                pltpu.VMEM((SLOTS, part, cols), bf16),
                pltpu.VMEM((len(UNITS), 16, tokens), bf16),
                pltpu.VMEM((len(GROUPED), RING, 16, part), bf16),
                pltpu.VMEM((n_part, RING, 16, cols), f32),
                pltpu.VMEM((n_part, RING - 1, 16, cols), f32),
                pltpu.VMEM((16, 16, cols), f32),
                pltpu.VMEM(w_qkv.shape, f32),
                pltpu.VMEM(w_out.shape, f32),
                pltpu.VMEM(r_qkv.shape, f32),
                pltpu.VMEM(c_qkv.shape, f32),
                pltpu.VMEM(r_out.shape, f32),
                pltpu.VMEM(c_out.shape, f32),
                pltpu.VMEM((n_b, 16, 128), f32),
                pltpu.VMEM((n_b, 16, 128), f32),
                pltpu.VMEM((n_b, 2, CUBE, most, 128), f32),
                pltpu.VMEM((n_b, most, 128), f32),
                pltpu.VMEM((n_b, most, 128), f32),
                pltpu.VMEM((8, 128), f32),
                pltpu.VMEM((n_b, 16, 128), f32),
                pltpu.VMEM((n_b, most, 128), f32),
                dma((6,)),
                dma((len(UNITS),)),
                dma((len(BLOCKS),)),
                dma((len(GROUPED), RING - 1)),
                dma((len(GROUPED), RING - 1)),
                dma((len(GROUPED), RING - 1)),
                dma((len(GROUPED), RING - 1)),
                dma((n_part, RING - 1)),
                dma((n_part, RING - 1)),
                dma((n_b,)),
                dma((n_b,)),
                dma((n_b, 2, CUBE - 1)),
                dma((n_b, 2, CUBE - 1)),
                dma((n_b,)),
                dma((n_b,)),
                dma((20,)),
            ],
            compiler_params=pltpu.CompilerParams(
                collective_id=0, has_side_effects=True, vmem_limit_bytes=64 * 1024 * 1024 - 64 * 1024
            ),
            name="adafactor",
        )(w_qkv, w_out, x_in, dy_qkv, x_attn, dy_out, r_qkv, c_qkv, r_out, c_out, hyper_params)
        out = pl.pallas_call(
            emit,
            out_shape=tuple(jax.ShapeDtypeStruct(a.shape, a.dtype) for a in out),
            in_specs=[pl.BlockSpec(memory_space=pl.ANY)] * len(out),
            out_specs=tuple(pl.BlockSpec(memory_space=pl.ANY) for _ in out),
            scratch_shapes=[pltpu.VMEM(a.shape, a.dtype) for a in out] + [dma((2, len(out)))],
            name="emit",
        )(*out)
        return (
            out[0],
            jnp.swapaxes(out[1], 1, 2),
            jnp.swapaxes(out[2], 0, 1),
            jnp.swapaxes(out[3], 0, 1),
            out[4],
            out[5],
        )

    return jax.shard_map(local_run, mesh=mesh, in_specs=in_specs, out_specs=out_specs, check_vma=False)
```
